128 devices in a mesh: gx: 8 (over y, x_hi), gy: 4 (over x_lo, core), gz: 4 (over z).
Axes of the slice: x: 4 (x_hi: 2, x_lo: 2; x = x_hi * 2 + x_lo), y: 4, z: 4, core: 2. Of those that a mesh axis runs over, the one named last changes fastest.
Arguments:
- right_side: float32 [64, 128, 1024], P('gx', 'gy', 'gz'), may hold values from -60 to 60
- wavenumber_sq: float32 [64, 128, 1024], P('gx', 'gy', 'gz'), may hold values from 0.3 to 1.5
- sketch_matrix: float32 [16, 64, 128, 1024], P(None, 'gx', 'gy', 'gz'), may hold values from -1.5 to 1.5
Outputs:
- solution: float32 [64, 128, 1024], P('gx', 'gy', 'gz')
- residual: float32 [64, 128, 1024], P('gx', 'gy', 'gz')
The draws below stay inside these ranges and needn't reach their ends.
All inputs are finite; a program needn't handle non-finite values.
Results may differ from the reference program's by a relative error of at most 0.0003.
Values sent between devices are 32-bit elements; how exact they have to be, the bound alone decides.
No kernel may reach another device: no remote copies, remote signals or barrier semaphores. Data moves between devices by JAX's collectives and lax.ppermute only.
A program may use at most 64 MiB of HBM per device.

```python
import math
import jax
import jax.numpy as jnp
from jax import lax

SK = 16
SWEEPS = 3
ITERS = 3
NX = 64
NY = 128
NZ = 1024


def draw_right_side(key, part):
    first_key = jax.random.fold_in(key, 11)
    xcoord = jnp.arange(NX, dtype=jnp.float32) / NX
    ycoord = jnp.arange(NY, dtype=jnp.float32) / NY
    zcoord = jnp.arange(NZ, dtype=jnp.float32) / NZ
    ramp = (xcoord[:, None, None] + ycoord[None, :, None] + zcoord[None, None, :]) / 3.0
    growth = jnp.exp(math.log(3.0) * ramp)
    noise = jnp.clip(jax.random.normal(first_key, (NX, NY, NZ), jnp.float32), -6.0, 6.0)
    values = noise * growth
    return values.astype(jnp.float32)


def block_scale(key, extent, split, low, top_value):
    level = 1.0
    for axis_at, blocks in split:
        steps = jax.random.uniform(jax.random.fold_in(jax.random.fold_in(key, 6), axis_at), (blocks,), jnp.float32, low / len(split), top_value / len(split))
        level = level * jnp.repeat(jnp.exp(steps), extent[axis_at] // blocks).reshape((-1,) + (1,) * (len(extent) - 1 - axis_at))
    return level


def bell_draw(stream_key, extent, deviation, reach, split=(), kind=jnp.bfloat16):
    array = jax.random.normal(stream_key, extent, jnp.float32) * deviation
    if len(split) > 0:
        array = block_scale(stream_key, extent, split, -0.22, 0.18) * array
    return jnp.clip(array, min=-reach, max=reach).astype(kind)


def setup_inputs(seed: int = 0) -> dict:
    streams_of = jax.random.split(jax.random.key(seed), 4)
    right_side = draw_right_side(jax.random.fold_in(streams_of[3], 71), 0)
    wavenumber_sq = jnp.clip(jnp.exp(math.log(1.5) - 1.60943787 * jax.random.uniform(streams_of[1], (NX, NY, NZ), jnp.float32) ** block_scale(streams_of[1], (NX, NY, NZ), ((0, 8), (1, 4), (2, 4)), -0.2, 0.2)), 0.3, 1.5)
    sketch_matrix = bell_draw(streams_of[2], (SK, NX, NY, NZ), SK ** -0.5, 1.5, ((1, 8), (2, 4), (3, 4)), jnp.float32)
    return {"right_side": right_side, "wavenumber_sq": wavenumber_sq, "sketch_matrix": sketch_matrix}


HIGH = lax.Precision.HIGHEST

def neighbours(grid_field):
    total = jnp.roll(grid_field, 1, 0) + jnp.roll(grid_field, -1, 0)
    total = total + jnp.roll(grid_field, 1, 1) + jnp.roll(grid_field, -1, 1)
    total = total + jnp.roll(grid_field, 1, 2) + jnp.roll(grid_field, -1, 2)
    return total

def smoother(vector, wavenumber_sq):
    diagonal = 6.0 + wavenumber_sq
    result = vector / diagonal
    for sweep_idx in range(SWEEPS):
        result = result + (vector - (diagonal * result - neighbours(result))) / diagonal
    return result

def helmholtz(grid_field, wavenumber_sq):
    return (6.0 - wavenumber_sq) * grid_field - neighbours(grid_field)

def sketched(sketch_rows, grid_field):
    return jnp.dot(sketch_rows, grid_field.reshape(-1), precision=HIGH, preferred_element_type=jnp.float32)

def solve_small(hessen, beta_norm):
    target = jnp.zeros((ITERS + 1,), jnp.float32).at[0].set(beta_norm)
    basis = []
    upper = [[None] * ITERS for row_idx in range(ITERS)]
    for col_idx in range(ITERS):
        column = hessen[:, col_idx]
        for row_idx in range(col_idx):
            factor = jnp.sum(basis[row_idx] * column)
            upper[row_idx][col_idx] = factor
            column = column - factor * basis[row_idx]
        diag_term = jnp.sqrt(jnp.sum(column * column))
        upper[col_idx][col_idx] = diag_term
        basis.append(column / diag_term)
    projected = [jnp.sum(member * target) for member in basis]
    coeffs = [None] * ITERS
    for row_idx in reversed(range(ITERS)):
        accum = projected[row_idx]
        for col_idx in range(row_idx + 1, ITERS):
            accum = accum - upper[row_idx][col_idx] * coeffs[col_idx]
        coeffs[row_idx] = accum / upper[row_idx][row_idx]
    weights = jnp.stack(coeffs)
    leftover = target - jnp.dot(hessen, weights, precision=HIGH)
    return (weights, leftover)

def reference(right_side, wavenumber_sq, sketch_matrix):
    sketch_rows = sketch_matrix.reshape(SK, -1)
    rhs_sketch = sketched(sketch_rows, right_side)
    beta_norm = jnp.sqrt(jnp.sum(rhs_sketch * rhs_sketch))
    vectors = [right_side / beta_norm]
    images = [rhs_sketch / beta_norm]
    directions = []
    hessen = jnp.zeros((ITERS + 1, ITERS), jnp.float32)
    for iteration in range(ITERS):
        direction = smoother(vectors[-1], wavenumber_sq)
        directions.append(direction)
        product = helmholtz(direction, wavenumber_sq)
        sketch_new = sketched(sketch_rows, product)
        stacked = jnp.stack(images, axis=1)
        weights = jnp.dot(sketch_new, stacked, precision=HIGH)
        remainder = product
        for member in range(iteration + 1):
            remainder = remainder - weights[member] * vectors[member]
        sketch_rem = sketched(sketch_rows, remainder)
        length = jnp.sqrt(jnp.sum(sketch_rem * sketch_rem))
        vectors.append(remainder / length)
        images.append(sketch_rem / length)
        hessen = hessen.at[:iteration + 1, iteration].set(weights)
        hessen = hessen.at[iteration + 1, iteration].set(length)
    coeffs, leftover = solve_small(hessen, beta_norm)
    solution = directions[0] * coeffs[0]
    for member in range(1, ITERS):
        solution = solution + directions[member] * coeffs[member]
    residual = vectors[0] * leftover[0]
    for member in range(1, ITERS + 1):
        residual = residual + vectors[member] * leftover[member]
    return (solution, residual)
```

```python
import functools

import jax
import jax.numpy as jnp
from jax import lax
from jax.experimental import pallas as pl
from jax.experimental.pallas import tpu as pltpu
from jax.sharding import Mesh
from jax.sharding import PartitionSpec as P

SK = 16
SWEEPS = 3
ITERS = 3
RADIUS = 4
DEPTH = ITERS * RADIUS
BX, BY, BZ = 8, 32, 256
ROW0 = 24
ROWS = 80
LAYERS = BX + 2 * DEPTH
OWN = DEPTH
TILES = 3

VMEM = pltpu.VMEM
F32 = jnp.float32


def layer_of(part, idx):
    if part == "own":
        return OWN + idx
    if part == "twin":
        return OWN + 15 - idx
    if part == "relay":
        return OWN - 1 - idx
    if part == "outer_relay":
        return idx
    return OWN + 16 + idx


def distance(layer):
    return max(0, OWN - layer, layer - (OWN + BX - 1))


ALL_PARTS = (
    [("outer_relay", i) for i in range(4)]
    + [("relay", i) for i in range(8)]
    + [("own", i) for i in range(8)]
    + [("twin", i) for i in range(8)]
    + [("outer_twin", i) for i in range(4)]
)

FIRST = (
    [("A", ("own", i)) for i in range(8)]
    + [("A", ("twin", i)) for i in range(8)]
    + [("B", ("own", i), ("own", i + 1)) for i in (0, 2, 4, 6)]
    + [("B", ("twin", i), ("twin", i + 1)) for i in (4, 6)]
)
SECOND = (
    [("A", ("relay", i)) for i in range(8)]
    + [("B", ("relay", i), ("relay", i + 1)) for i in (0, 2)]
    + [
        ("C", ("outer_relay", 1), ("outer_relay", 2)),
        ("C", ("outer_relay", 3), ("outer_twin", 0)),
        ("C", ("outer_twin", 1), ("outer_twin", 2)),
    ]
)


def lane_plan():
    plan = {}
    place = [0, 0]
    order = sorted(ALL_PARTS, key=lambda part: distance(layer_of(*part)))
    for part in order:
        dist = distance(layer_of(*part))
        width = DEPTH - dist
        if width <= 0:
            continue
        tile = 0 if dist in (0, 1, 10, 11) else 1
        plan[part] = (tile, place[tile], width)
        place[tile] += width
    assert max(place) <= 128
    return plan


LANES = lane_plan()


def roll(value, shift, axis):
    shift = shift % value.shape[axis]
    if shift == 0:
        return value
    return pltpu.roll(value, shift, axis)


def prep_kernel(flip_ref, rhs_ref, coef_ref, out_ref):
    flip = flip_ref[0]
    for i in range(BX):
        source = jnp.where(flip == 1, BX - 1 - i, i)
        out_ref[0, i] = rhs_ref[source]
        out_ref[1, i] = 1.0 / (6.0 + coef_ref[source])


def pack_rows_kernel(slots, names, *refs):
    sources = dict(zip(names, refs))
    low_ref, high_ref = refs[len(names) :]
    sub = lax.broadcasted_iota(jnp.int32, (8, BZ), 0)
    for array in range(2):
        for slot, (kind, *parts) in enumerate(slots):
            values = []
            for tiles in ((0, 1), (3, 2)):
                tile = tiles[1] if kind == "B" else tiles[0]
                values.append([sources[p][array, i, tile * 8 : tile * 8 + 8] for p, i in parts])
            low, high = values
            if kind == "A":
                low_ref[array, slot] = low[0]
                high_ref[array, slot] = high[0]
            else:
                low_ref[array, slot] = jnp.where(sub < 4, low[0], roll(low[1], 4, 0))
                high_ref[array, slot] = jnp.where(sub >= 4, high[0], roll(high[1], 4, 0))


def row_sources(slots):
    found = {}
    for slot, (kind, *parts) in enumerate(slots):
        for at, part in enumerate(parts):
            below, above = (0, 7) if kind == "B" else (1, 6)
            found.setdefault(part, {})[below] = (slot, at)
            found.setdefault(part, {})[above] = (slot, at)
    return found


def halo_tile(message_ref, array, where, lane_tile):
    slot, rolled = where
    value = message_ref[array, slot, :, lane_tile * 128 : lane_tile * 128 + 128]
    return roll(value, 4, 0) if rolled else value


def assemble_kernel(*refs):
    names = ("own", "twin", "relay", "outer_relay", "outer_twin")
    sources = dict(zip(names, refs[:5]))
    below = (refs[5], refs[7])
    above = (refs[6], refs[8])
    ext_ref, low_ref, high_ref = refs[9:]
    first, second = row_sources(FIRST), row_sources(SECOND)
    lane = lax.broadcasted_iota(jnp.int32, (8, 128), 1)
    for array in range(2):
        for row_tile in range(8):
            packed = [[None, None], [None, None]]
            for part in ALL_PARTS:
                name, idx = part
                layer = layer_of(name, idx)
                tiles = []
                for lane_tile in range(2):
                    if 2 <= row_tile <= 5:
                        row = (row_tile - 2) * 8
                        value = sources[name][array, idx, row : row + 8, lane_tile * 128 : lane_tile * 128 + 128]
                    else:
                        message = 0 if part in first else 1
                        where = (first if message == 0 else second).get(part, {}).get(row_tile)
                        if where is None:
                            value = None
                        else:
                            side = below if row_tile < 2 else above
                            value = halo_tile(side[message], array, where, lane_tile)
                    if value is not None:
                        row = 8 + row_tile * 8
                        ext_ref[array, lane_tile, layer, row : row + 8] = value
                    tiles.append(value)
                if part in LANES and tiles[0] is not None:
                    tile, place, width = LANES[part]
                    mask = (lane >= place) & (lane < place + width)
                    low = roll(tiles[0], place, 1)
                    high = roll(tiles[1], place + width, 1)
                    for side, value in ((0, low), (1, high)):
                        old = packed[side][tile]
                        packed[side][tile] = value if old is None else jnp.where(mask, value, old)
            for tile in range(2):
                for side, out_ref in ((0, low_ref), (1, high_ref)):
                    value = packed[side][tile]
                    if value is not None:
                        out_ref[array, tile, row_tile * 8 : row_tile * 8 + 8] = value


def neighbours(ref, layer, row, tiles, lane):
    here = [ref[t, layer, row : row + 8] for t in range(TILES)]
    up = [roll(v, 127, 1) for v in here]
    down = [roll(v, 1, 1) for v in here]
    sums = []
    for t in tiles:
        total = ref[t, layer - 1, row : row + 8] + ref[t, layer + 1, row : row + 8]
        total = total + (ref[t, layer, row - 1 : row + 7] + ref[t, layer, row + 1 : row + 9])
        along = jnp.where(lane == 127, up[(t + 1) % TILES], up[t])
        along = along + jnp.where(lane == 0, down[(t + 2) % TILES], down[t])
        sums.append(total + along)
    return here, sums


def rows_of(reach):
    if reach == 0:
        return range(2, 6)
    return range(1, 7) if reach <= 8 else range(0, 8)


def main_kernel(
    flip_ref, sketch_hbm, ext_ref, below_ref, above_ref, vectors_ref, images_ref,
    vec, inv, za, zb, mid, sketch, sem,
):
    copy = pltpu.make_async_copy(sketch_hbm, sketch, sem)
    copy.start()
    flip = flip_ref[0]
    lane = lax.broadcasted_iota(jnp.int32, (8, 128), 1)

    for array, target in ((0, vec), (1, inv)):
        for part in LANES:
            tile, place, width = LANES[part]
            layer = layer_of(*part)
            for row_tile in rows_of(DEPTH) if distance(layer) <= 3 else rows_of(8):
                row = row_tile * 8
                low = roll(above_ref[array, tile, row : row + 8], -place, 1)
                high = roll(below_ref[array, tile, row : row + 8], -(place + width), 1)
                target[2, layer, row + 8 : row + 16] = jnp.where(lane < 64, low, high)

    def copy_layer(layer, _):
        for row_tile in range(8):
            row = 8 + row_tile * 8
            for t in range(2):
                value = ext_ref[0, t, layer, row : row + 8]
                scale = ext_ref[1, t, layer, row : row + 8]
                vec[t, layer, row : row + 8] = value
                inv[t, layer, row : row + 8] = scale
                za[t, layer, row : row + 8] = value * scale
            za[2, layer, row : row + 8] = vec[2, layer, row : row + 8] * inv[2, layer, row : row + 8]
        return 0

    lax.fori_loop(0, LAYERS, copy_layer, 0)

    for step in range(ITERS):
        reach = DEPTH - step * RADIUS

        def sweep(source, target, left, keep):
            def body(layer, _):
                for row_tile in rows_of(left):
                    row = 8 + row_tile * 8
                    _, sums = neighbours(source, layer, row, range(TILES), lane)
                    for t in range(TILES):
                        total = vec[t, layer, row : row + 8] + sums[t]
                        if keep:
                            mid[t, layer, row : row + 8] = total
                        target[t, layer, row : row + 8] = total * inv[t, layer, row : row + 8]
                return 0

            lax.fori_loop(OWN - left, OWN + BX + left, body, 0)

        sweep(za, zb, reach - 1, False)
        sweep(zb, za, reach - 2, False)
        sweep(za, zb, reach - 3, True)
        left = reach - 4
        last = step == ITERS - 1

        def apply(layer, _):
            for row_tile in rows_of(left):
                row = 8 + row_tile * 8
                tiles = range(2) if last else range(TILES)
                here, sums = neighbours(zb, layer, row, tiles, lane)
                for t in tiles:
                    value = 12.0 * here[t] - mid[t, layer, row : row + 8] - sums[t]
                    vec[t, layer, row : row + 8] = value
                    if not last:
                        za[t, layer, row : row + 8] = value * inv[t, layer, row : row + 8]
            return 0

        lax.fori_loop(OWN - left, OWN + BX + left, apply, 0)

        def keep_own(i, _):
            natural = jnp.where(flip == 1, BX - 1 - i, i)
            for row in range(0, BY, 8):
                for t in range(2):
                    cols = slice(t * 128, t * 128 + 128)
                    at = slice(ROW0 + row, ROW0 + row + 8)
                    vectors_ref[step + 1, natural, row : row + 8, cols] = vec[t, OWN + i, at]
                    vectors_ref[4 + step, natural, row : row + 8, cols] = zb[t, OWN + i, at]
            return 0

        if step == 0:

            def keep_first(i, _):
                natural = jnp.where(flip == 1, BX - 1 - i, i)
                for row in range(0, BY, 8):
                    for t in range(2):
                        cols = slice(t * 128, t * 128 + 128)
                        at = slice(ROW0 + row, ROW0 + row + 8)
                        vectors_ref[0, natural, row : row + 8, cols] = ext_ref[0, t, OWN + i, at]
                return 0

            lax.fori_loop(0, BX, keep_first, 0)
        lax.fori_loop(0, BX, keep_own, 0)

    copy.wait()
    group = 4
    totals = []
    for start in range(0, SK, group):

        def body(i, carry):
            carry = list(carry)
            for row in range(0, BY, 8):
                for t in range(2):
                    cols = slice(t * 128, t * 128 + 128)
                    fields = [vectors_ref[j, i, row : row + 8, cols] for j in range(4)]
                    for s in range(group):
                        weight = sketch[start + s, i, row : row + 8, cols]
                        for j in range(4):
                            carry[j * group + s] = carry[j * group + s] + weight * fields[j]
            return tuple(carry)

        zero = jnp.zeros((8, 128), F32)
        totals.append(lax.fori_loop(0, BX, body, (zero,) * (4 * group)))
    lanes = lax.broadcasted_iota(jnp.int32, (1, 128), 1)
    image = jnp.zeros((1, 128), F32)
    for g, sums in enumerate(totals):
        for j in range(4):
            for s in range(group):
                value = jnp.sum(jnp.sum(sums[j * group + s], axis=0, keepdims=True), axis=1, keepdims=True)
                image = jnp.where(lanes == j * SK + g * group + s, value, image)
    images_ref[...] = jnp.broadcast_to(image, images_ref.shape)


def dot(left, right):
    return jnp.sum(left * right, axis=0, keepdims=True)


def small_solve(totals):
    row = lax.broadcasted_iota(jnp.int32, (4 * SK, 128), 0)
    col = lax.broadcasted_iota(jnp.int32, (4 * SK, 128), 1)
    wide = jnp.where(row == col, jnp.broadcast_to(totals, (4 * SK, 128)), 0.0)
    spread = jnp.broadcast_to(jnp.sum(wide, axis=1, keepdims=True), (4 * SK, 128))
    sketches = [spread[j * SK : (j + 1) * SK] for j in range(4)]
    zero = jnp.zeros((1, 128), F32)
    beta = jnp.sqrt(dot(sketches[0], sketches[0]))
    basis = [[1.0 / beta, zero, zero, zero]]
    images = [sketches[0] / beta]
    hessen = [[zero] * ITERS for _ in range(ITERS + 1)]
    for j in range(ITERS):
        combo = [zero] + [basis[j][i] for i in range(3)]
        image = combo[1] * sketches[1]
        for i in range(1, j + 1):
            image = image + combo[i + 1] * sketches[i + 1]
        weights = [dot(member, image) for member in images]
        rest = image
        for i in range(j + 1):
            rest = rest - weights[i] * images[i]
            combo = [combo[k] - weights[i] * basis[i][k] for k in range(4)]
            hessen[i][j] = weights[i]
        length = jnp.sqrt(dot(rest, rest))
        hessen[j + 1][j] = length
        basis.append([entry / length for entry in combo])
        images.append(rest / length)
    target = [beta, zero, zero, zero]

    def inner(left, right):
        total = left[0] * right[0]
        for a, b in zip(left[1:], right[1:]):
            total = total + a * b
        return total

    members = []
    upper = [[None] * ITERS for _ in range(ITERS)]
    for j in range(ITERS):
        column = [hessen[i][j] for i in range(ITERS + 1)]
        for i in range(j):
            factor = inner(members[i], column)
            upper[i][j] = factor
            column = [c - factor * m for c, m in zip(column, members[i])]
        diag = jnp.sqrt(inner(column, column))
        upper[j][j] = diag
        members.append([c / diag for c in column])
    coeffs = [None] * ITERS
    for j in reversed(range(ITERS)):
        accum = inner(members[j], target)
        for i in range(j + 1, ITERS):
            accum = accum - upper[j][i] * coeffs[i]
        coeffs[j] = accum / upper[j][j]
    leftover = []
    for i in range(ITERS + 1):
        total = hessen[i][0] * coeffs[0]
        for j in range(1, ITERS):
            total = total + hessen[i][j] * coeffs[j]
        leftover.append(target[i] - total)
    for_images = []
    for i in range(ITERS):
        total = coeffs[0] * basis[0][i]
        for j in range(1, ITERS):
            total = total + coeffs[j] * basis[j][i]
        for_images.append(total)
    for_vectors = []
    for i in range(ITERS + 1):
        total = leftover[0] * basis[0][i]
        for j in range(1, ITERS + 1):
            total = total + leftover[j] * basis[j][i]
        for_vectors.append(total)
    return for_images, for_vectors


def final_kernel(sums_ref, vectors_ref, solution_ref, residual_ref):
    totals = jnp.sum(sums_ref[...], axis=0, keepdims=True)
    for_images, for_vectors = small_solve(totals)
    for_images = [jnp.broadcast_to(w, (8, 128)) for w in for_images]
    for_vectors = [jnp.broadcast_to(w, (8, 128)) for w in for_vectors]

    def body(i, _):
        for row in range(0, BY, 8):
            for t in range(2):
                at = (i, slice(row, row + 8), slice(t * 128, t * 128 + 128))
                total = for_images[0] * vectors_ref[(4, *at)]
                for j in range(1, ITERS):
                    total = total + for_images[j] * vectors_ref[(4 + j, *at)]
                solution_ref[at] = total
                total = for_vectors[0] * vectors_ref[(0, *at)]
                for j in range(1, ITERS + 1):
                    total = total + for_vectors[j] * vectors_ref[(j, *at)]
                residual_ref[at] = total
        return 0

    lax.fori_loop(0, BX, body, 0)


def vmem(count):
    return [pl.BlockSpec(memory_space=VMEM)] * count


SMEM_SPEC = pl.BlockSpec(memory_space=pltpu.SMEM)


def struct(*shape):
    return jax.ShapeDtypeStruct(shape, F32)


def params(mib):
    return pltpu.CompilerParams(vmem_limit_bytes=mib << 20)


def local(right_side, wavenumber_sq, sketch_matrix):
    flip = lax.axis_index("xh").astype(jnp.int32).reshape(1)
    block = pl.pallas_call(
        prep_kernel,
        out_shape=struct(2, BX, BY, BZ),
        in_specs=[SMEM_SPEC] + vmem(2),
        out_specs=vmem(1)[0],
        compiler_params=params(8),
        name="prep",
    )(flip, right_side, wavenumber_sq)

    pairs = [(y * 2 + h, (y + (1 - 2 * h)) % 4 * 2 + h) for y in range(4) for h in range(2)]
    back = [(b, a) for a, b in pairs]
    around = [(i, (i + 1) % 4) for i in range(4)]
    inverse = [(b, a) for a, b in around]
    twin = lax.ppermute(block, "xh", [(0, 1), (1, 0)])
    outer_relay = lax.ppermute(block[:, 4:], ("y", "xh"), pairs)
    outer_twin = lax.ppermute(block[:, :4], ("y", "xh"), back)
    relay = lax.ppermute(twin, ("y", "xh"), pairs)

    def pack(slots, names, *parts):
        count = len(slots)
        low, high = pl.pallas_call(
            functools.partial(pack_rows_kernel, slots, names),
            out_shape=[struct(2, count, 8, BZ)] * 2,
            in_specs=vmem(len(parts)),
            out_specs=vmem(2),
            compiler_params=params(8),
            name="pack_rows",
        )(*parts)
        above = lax.ppermute(low, ("xl", "co"), inverse)
        below = lax.ppermute(high, ("xl", "co"), around)
        return below, above

    below_1, above_1 = pack(FIRST, ("own", "twin"), block, twin)
    below_2, above_2 = pack(
        SECOND, ("relay", "outer_relay", "outer_twin"), relay, outer_relay, outer_twin
    )
    ext, low, high = pl.pallas_call(
        assemble_kernel,
        out_shape=[struct(2, 2, LAYERS, ROWS, 128), struct(2, 2, 64, 128), struct(2, 2, 64, 128)],
        in_specs=vmem(9),
        out_specs=vmem(3),
        compiler_params=params(16),
        name="assemble",
    )(block, twin, relay, outer_relay, outer_twin, below_1, above_1, below_2, above_2)
    above = lax.ppermute(low, "z", inverse)
    below = lax.ppermute(high, "z", around)

    field = VMEM((TILES, LAYERS, ROWS, 128), F32)
    vectors, images = pl.pallas_call(
        main_kernel,
        out_shape=[struct(7, BX, BY, BZ), struct(128, 128)],
        in_specs=[SMEM_SPEC, pl.BlockSpec(memory_space=pl.ANY)] + vmem(3),
        out_specs=vmem(2),
        scratch_shapes=[field] * 5 + [VMEM((SK, BX, BY, BZ), F32), pltpu.SemaphoreType.DMA],
        compiler_params=params(40),
        name="krylov",
    )(flip, sketch_matrix, ext, below, above)

    sums = lax.all_to_all(images, ("y", "xh", "xl", "co", "z"), 0, 0, tiled=True)
    return tuple(
        pl.pallas_call(
            final_kernel,
            out_shape=[struct(BX, BY, BZ)] * 2,
            in_specs=vmem(2),
            out_specs=vmem(2),
            compiler_params=params(8),
            name="combine",
        )(sums, vectors)
    )


def solution(mesh):
    finer = Mesh(mesh.devices.reshape(4, 2, 2, 2, 4), ("y", "xh", "xl", "co", "z"))
    spec = (("y", "xh"), ("xl", "co"), "z")
    return jax.shard_map(
        local,
        mesh=finer,
        in_specs=(P(*spec), P(*spec), P(None, *spec)),
        out_specs=(P(*spec), P(*spec)),
        check_vma=False,
    )
```

```python
import functools

import jax
import jax.numpy as jnp
from jax import lax
from jax.experimental import pallas as pl
from jax.experimental.pallas import tpu as pltpu
from jax.sharding import Mesh
from jax.sharding import PartitionSpec as P

SK = 16
SWEEPS = 3
ITERS = 3
RADIUS = 4
DEPTH = ITERS * RADIUS
BX, BY, BZ = 8, 32, 256
ROW0 = 24
ROWS = 80
LAYERS = BX + 2 * DEPTH
OWN = DEPTH

VMEM = pltpu.VMEM
F32 = jnp.float32


def layer_of(part, idx):
    if part == "own":
        return OWN + idx
    if part == "twin":
        return OWN + 15 - idx
    if part == "relay":
        return OWN - 1 - idx
    if part == "outer_relay":
        return idx
    return OWN + 16 + idx


def distance(layer):
    return max(0, OWN - layer, layer - (OWN + BX - 1))


ALL_PARTS = (
    [("outer_relay", i) for i in range(4)]
    + [("relay", i) for i in range(8)]
    + [("own", i) for i in range(8)]
    + [("twin", i) for i in range(8)]
    + [("outer_twin", i) for i in range(4)]
)

FIRST = (
    [("A", ("own", i)) for i in range(8)]
    + [("A", ("twin", i)) for i in range(8)]
    + [("B", ("own", i), ("own", i + 1)) for i in (0, 2, 4, 6)]
    + [("B", ("twin", i), ("twin", i + 1)) for i in (4, 6)]
)
SECOND = (
    [("A", ("relay", i)) for i in range(8)]
    + [("B", ("relay", i), ("relay", i + 1)) for i in (0, 2)]
    + [
        ("C", ("outer_relay", 1), ("outer_relay", 2)),
        ("C", ("outer_relay", 3), ("outer_twin", 0)),
        ("C", ("outer_twin", 1), ("outer_twin", 2)),
    ]
)


def lane_plan():
    plan = {}
    for tile, dists in enumerate((range(2), range(2, DEPTH))):
        order = [part for part in ALL_PARTS if distance(layer_of(*part)) in dists]
        order.sort(key=lambda part: -distance(layer_of(*part)))
        place, before = 0, 0
        for part in order:
            width = DEPTH - distance(layer_of(*part))
            place += max(width, before)
            before = width
            plan[part] = (tile, place, width)
        first = DEPTH - distance(layer_of(*order[0]))
        assert place + max(before, first) - first <= 128
    return plan


LANES = lane_plan()


def roll(value, shift, axis):
    shift = shift % value.shape[axis]
    if shift == 0:
        return value
    return pltpu.roll(value, shift, axis)


def prep_kernel(flip_ref, rhs_ref, coef_ref, out_ref):
    flip = flip_ref[0]
    for i in range(BX):
        source = jnp.where(flip == 1, BX - 1 - i, i)
        out_ref[0, i] = rhs_ref[source]
        out_ref[1, i] = 1.0 / (6.0 + coef_ref[source])


def pack_rows_kernel(slots, names, *refs):
    sources = dict(zip(names, refs))
    low_ref, high_ref = refs[len(names) :]
    sub = lax.broadcasted_iota(jnp.int32, (8, BZ), 0)
    for array in range(2):
        for slot, (kind, *parts) in enumerate(slots):
            values = []
            for tiles in ((0, 1), (3, 2)):
                tile = tiles[1] if kind == "B" else tiles[0]
                values.append([sources[p][array, i, tile * 8 : tile * 8 + 8] for p, i in parts])
            low, high = values
            if kind == "A":
                low_ref[array, slot] = low[0]
                high_ref[array, slot] = high[0]
            else:
                low_ref[array, slot] = jnp.where(sub < 4, low[0], roll(low[1], 4, 0))
                high_ref[array, slot] = jnp.where(sub >= 4, high[0], roll(high[1], 4, 0))


def row_sources(slots):
    found = {}
    for slot, (kind, *parts) in enumerate(slots):
        for at, part in enumerate(parts):
            below, above = (0, 7) if kind == "B" else (1, 6)
            found.setdefault(part, {})[below] = (slot, at)
            found.setdefault(part, {})[above] = (slot, at)
    return found


def halo_tile(message_ref, array, where, lane_tile):
    slot, rolled = where
    value = message_ref[array, slot, :, lane_tile * 128 : lane_tile * 128 + 128]
    return roll(value, 4, 0) if rolled else value


PART_NAMES = ("own", "twin", "relay", "outer_relay", "outer_twin")
FOUND = (row_sources(FIRST), row_sources(SECOND))


class Blocks:
    def __init__(self, refs):
        self.sources = dict(zip(PART_NAMES, refs[:5]))
        self.below = (refs[5], refs[7])
        self.above = (refs[6], refs[8])

    def tile(self, array, part, row_tile, lane_tile):
        cols = slice(lane_tile * 128, lane_tile * 128 + 128)
        if 2 <= row_tile <= 5:
            name, idx = part
            return self.sources[name][array, idx, row_tile * 8 - 16 : row_tile * 8 - 8, cols]
        message = 0 if part in FOUND[0] else 1
        where = FOUND[message].get(part, {}).get(row_tile)
        if where is None:
            return None
        side = self.below if row_tile < 2 else self.above
        return halo_tile(side[message], array, where, lane_tile)


def pack_columns_kernel(*refs):
    blocks = Blocks(refs)
    low_ref, high_ref = refs[9:]
    lane = lax.broadcasted_iota(jnp.int32, (8, 128), 1)
    for array in range(2):
        for row_tile in range(8):
            low, high = [None, None], [None, None]
            for part, (tile, place, width) in LANES.items():
                first = blocks.tile(array, part, row_tile, 0)
                if first is None:
                    continue
                value = roll(first, place + 64, 1)
                start = (place + 64) % 128
                if start + width <= 128:
                    mask = (lane >= start) & (lane < start + width)
                else:
                    mask = (lane >= start) | (lane < start + width - 128)
                low[tile] = value if low[tile] is None else jnp.where(mask, value, low[tile])
                value = roll(blocks.tile(array, part, row_tile, 1), place, 1)
                mask = (lane >= place - width) & (lane < place)
                high[tile] = value if high[tile] is None else jnp.where(mask, value, high[tile])
            for tile in range(2):
                for value, out_ref in ((low[tile], low_ref), (high[tile], high_ref)):
                    if value is not None:
                        out_ref[array, tile, row_tile * 8 : row_tile * 8 + 8] = value


def rows_of(reach):
    if reach == 0:
        return range(2, 6)
    return range(1, 7) if reach <= 8 else range(0, 8)


def over_layers(first, count, group, body):
    whole, rest = divmod(count, group)

    def step(i, _):
        body(first + i * group, group)
        return 0

    if whole == 1:
        body(first, group)
    elif whole > 1:
        lax.fori_loop(0, whole, step, 0)
    if rest:
        body(first + whole * group, rest)


def neighbour_sums(ref, layer, count, row, tiles, lane, out):
    here = {(l, t): ref[t, layer + l, row : row + 8] for l in range(-1, count + 1) for t in range(tiles)}
    for l in range(count):
        ups = [roll(here[l, t], 127, 1) for t in range(tiles)]
        downs = [roll(here[l, t], 1, 1) for t in range(tiles)]
        if tiles == 2:
            ups = [jnp.where(lane == 127, ups[1 - t], ups[t]) for t in range(2)]
            downs = [jnp.where(lane == 0, downs[1 - t], downs[t]) for t in range(2)]
        for t in range(tiles):
            total = here[l - 1, t] + here[l + 1, t]
            total = total + (ref[t, layer + l, row - 1 : row + 7] + ref[t, layer + l, row + 1 : row + 9])
            out(l, t, here[l, t], total + (ups[t] + downs[t]))


def krylov_steps(vec, inv, za, zb, mid, tiles, group, lane, keep_own):
    for step in range(ITERS):
        reach = DEPTH - step * RADIUS

        def sweep(source, target, left, keep):
            def body(layer, count):
                for row_tile in rows_of(left):
                    row = 8 + row_tile * 8

                    def out(l, t, here, total):
                        total = total + vec[t, layer + l, row : row + 8]
                        if keep:
                            mid[t, layer + l, row : row + 8] = total
                        target[t, layer + l, row : row + 8] = total * inv[t, layer + l, row : row + 8]

                    neighbour_sums(source, layer, count, row, tiles, lane, out)

            over_layers(OWN - left, BX + 2 * left, group, body)

        sweep(za, zb, reach - 1, False)
        sweep(zb, za, reach - 2, False)
        sweep(za, zb, reach - 3, True)
        left = reach - 4
        last = step == ITERS - 1

        def apply(layer, count):
            for row_tile in rows_of(left):
                row = 8 + row_tile * 8

                def out(l, t, here, total):
                    value = 12.0 * here - mid[t, layer + l, row : row + 8] - total
                    vec[t, layer + l, row : row + 8] = value
                    if not last:
                        za[t, layer + l, row : row + 8] = value * inv[t, layer + l, row : row + 8]

                neighbour_sums(zb, layer, count, row, tiles, lane, out)

        over_layers(OWN - left, BX + 2 * left, group, apply)
        keep_own(step)


def sketch_sums(sums_ref, start_ref, sketch_ref, field_of, first, width):
    group = 4
    fields = range(first, 4)
    for start in range(0, SK, group):

        def body(i, carry):
            carry = list(carry)
            for row in range(0, BY, 8):
                for t in range(width):
                    cols = slice(t * 128, t * 128 + 128)
                    values = [field_of(j, i, row, t) for j in fields]
                    for s in range(group):
                        weight = sketch_ref[start + s, i, row : row + 8, cols]
                        for j, value in enumerate(values):
                            carry[j * group + s] = carry[j * group + s] + weight * value
            return tuple(carry)

        at = [(j * SK + start + s) for j in fields for s in range(group)]
        if start_ref is None:
            zero = jnp.zeros((8, 128), F32)
            init = (zero,) * len(at)
        else:
            init = tuple(start_ref[k] for k in at)
        for k, value in zip(at, lax.fori_loop(0, BX, body, init)):
            sums_ref[k] = value


def interior_kernel(flip_ref, sketch, *refs):
    blocks = Blocks(refs[:9])
    vectors_ref, sums_ref, edge_ref, thin_ref, vec, inv, za, zb, mid = refs[9:]
    flip = flip_ref[0]
    lane = lax.broadcasted_iota(jnp.int32, (8, 128), 1)

    for part in ALL_PARTS:
        layer = layer_of(*part)
        for row_tile in range(8):
            row = 8 + row_tile * 8
            if blocks.tile(0, part, row_tile, 0) is None:
                continue
            values = [[blocks.tile(array, part, row_tile, t) for t in range(2)] for array in range(2)]
            for t in range(2):
                vec[t, layer, row : row + 8] = values[0][t]
                inv[t, layer, row : row + 8] = values[1][t]
                za[t, layer, row : row + 8] = values[0][t] * values[1][t]
            for array in range(2):
                edge_ref[array, layer, row : row + 8] = jnp.where(
                    lane < 32, values[array][0], roll(values[array][1], 64, 1)
                )

    def natural(i):
        return jnp.where(flip == 1, BX - 1 - i, i)

    def own(source, place):
        def body(i, _):
            for row in range(0, BY, 8):
                for t in range(2):
                    vectors_ref[place, natural(i), row : row + 8, t * 128 : t * 128 + 128] = source[
                        t, OWN + i, ROW0 + row : ROW0 + row + 8
                    ]
            return 0

        lax.fori_loop(0, BX, body, 0)

    own(vec, 0)

    def keep_own(step):
        own(vec, 1 + step)
        own(zb, 4 + step)

    krylov_steps(vec, inv, za, zb, mid, 2, 2, lane, keep_own)

    def field_of(j, i, row, t):
        value = vectors_ref[j, i, row : row + 8, t * 128 : t * 128 + 128]
        if j == 0:
            return value
        return jnp.where(lane >= DEPTH if t == 0 else lane < 128 - DEPTH, value, 0.0)

    sketch_sums(sums_ref, None, sketch, field_of, 0, 2)

    def thin(i, _):
        for s in range(SK):
            for row in range(0, BY, 8):
                left = sketch[s, i, row : row + 8, 0:128]
                right = roll(sketch[s, i, row : row + 8, 128:256], 64, 1)
                thin_ref[s, i, row : row + 8] = jnp.where(lane < 32, left, right)
        return 0

    lax.fori_loop(0, BX, thin, 0)


def edge_kernel(flip_ref, edge_ref, below_ref, above_ref, thin_ref, before_ref, vectors_ref, images_ref, vec, inv, za, zb, mid, sums):
    flip = flip_ref[0]
    lane = lax.broadcasted_iota(jnp.int32, (8, 128), 1)

    for part, (tile, place, width) in LANES.items():
        layer = layer_of(*part)
        mask = (lane >= place - width) & (lane < place)
        for row_tile in rows_of(DEPTH) if distance(layer) <= 3 else rows_of(8):
            at = slice(8 + row_tile * 8, 16 + row_tile * 8)
            values = []
            for array in range(2):
                rows = slice(row_tile * 8, row_tile * 8 + 8)
                halo = jnp.where(mask, below_ref[array, tile, rows], above_ref[array, tile, rows])
                values.append(jnp.where(lane < 64, edge_ref[array, layer, at], roll(halo, -place, 1)))
            vec[0, layer, at] = values[0]
            inv[0, layer, at] = values[1]
            za[0, layer, at] = values[0] * values[1]

    def natural(i):
        return jnp.where(flip == 1, BX - 1 - i, i)

    def own(source, place):
        def body(i, _):
            for row in range(0, BY, 8):
                vectors_ref[place, natural(i), row : row + 8] = source[0, OWN + i, ROW0 + row : ROW0 + row + 8]
            return 0

        lax.fori_loop(0, BX, body, 0)

    own(vec, 0)

    def keep_own(step):
        own(vec, 1 + step)
        own(zb, 4 + step)

    krylov_steps(vec, inv, za, zb, mid, 1, 6, lane, keep_own)

    inside = (lane < DEPTH) | ((lane >= 64 - DEPTH) & (lane < 64))

    def field_of(j, i, row, t):
        return jnp.where(inside, vectors_ref[j, i, row : row + 8], 0.0)

    sketch_sums(sums, before_ref, thin_ref, field_of, 1, 1)
    lanes = lax.broadcasted_iota(jnp.int32, (1, 128), 1)
    image = jnp.zeros((1, 128), F32)
    for k in range(4 * SK):
        value = sums[k] if k >= SK else before_ref[k]
        value = jnp.sum(jnp.sum(value, axis=0, keepdims=True), axis=1, keepdims=True)
        image = jnp.where(lanes == k, value, image)
    images_ref[...] = jnp.broadcast_to(image, images_ref.shape)


def dot(left, right):
    return jnp.sum(left * right, axis=0, keepdims=True)


def small_solve(totals):
    row = lax.broadcasted_iota(jnp.int32, (4 * SK, 128), 0)
    col = lax.broadcasted_iota(jnp.int32, (4 * SK, 128), 1)
    wide = jnp.where(row == col, jnp.broadcast_to(totals, (4 * SK, 128)), 0.0)
    spread = jnp.broadcast_to(jnp.sum(wide, axis=1, keepdims=True), (4 * SK, 128))
    sketches = [spread[j * SK : (j + 1) * SK] for j in range(4)]
    zero = jnp.zeros((1, 128), F32)
    beta = jnp.sqrt(dot(sketches[0], sketches[0]))
    basis = [[1.0 / beta, zero, zero, zero]]
    images = [sketches[0] / beta]
    hessen = [[zero] * ITERS for _ in range(ITERS + 1)]
    for j in range(ITERS):
        combo = [zero] + [basis[j][i] for i in range(3)]
        image = combo[1] * sketches[1]
        for i in range(1, j + 1):
            image = image + combo[i + 1] * sketches[i + 1]
        weights = [dot(member, image) for member in images]
        rest = image
        for i in range(j + 1):
            rest = rest - weights[i] * images[i]
            combo = [combo[k] - weights[i] * basis[i][k] for k in range(4)]
            hessen[i][j] = weights[i]
        length = jnp.sqrt(dot(rest, rest))
        hessen[j + 1][j] = length
        basis.append([entry / length for entry in combo])
        images.append(rest / length)
    target = [beta, zero, zero, zero]

    def inner(left, right):
        total = left[0] * right[0]
        for a, b in zip(left[1:], right[1:]):
            total = total + a * b
        return total

    members = []
    upper = [[None] * ITERS for _ in range(ITERS)]
    for j in range(ITERS):
        column = [hessen[i][j] for i in range(ITERS + 1)]
        for i in range(j):
            factor = inner(members[i], column)
            upper[i][j] = factor
            column = [c - factor * m for c, m in zip(column, members[i])]
        diag = jnp.sqrt(inner(column, column))
        upper[j][j] = diag
        members.append([c / diag for c in column])
    coeffs = [None] * ITERS
    for j in reversed(range(ITERS)):
        accum = inner(members[j], target)
        for i in range(j + 1, ITERS):
            accum = accum - upper[j][i] * coeffs[i]
        coeffs[j] = accum / upper[j][j]
    leftover = []
    for i in range(ITERS + 1):
        total = hessen[i][0] * coeffs[0]
        for j in range(1, ITERS):
            total = total + hessen[i][j] * coeffs[j]
        leftover.append(target[i] - total)
    for_images = []
    for i in range(ITERS):
        total = coeffs[0] * basis[0][i]
        for j in range(1, ITERS):
            total = total + coeffs[j] * basis[j][i]
        for_images.append(total)
    for_vectors = []
    for i in range(ITERS + 1):
        total = leftover[0] * basis[0][i]
        for j in range(1, ITERS + 1):
            total = total + leftover[j] * basis[j][i]
        for_vectors.append(total)
    return for_images, for_vectors


def final_kernel(sums_ref, vectors_ref, edges_ref, solution_ref, residual_ref):
    totals = jnp.sum(sums_ref[...], axis=0, keepdims=True)
    for_images, for_vectors = small_solve(totals)
    for_images = [jnp.broadcast_to(w, (8, 128)) for w in for_images]
    for_vectors = [jnp.broadcast_to(w, (8, 128)) for w in for_vectors]
    lane = lax.broadcasted_iota(jnp.int32, (8, 128), 1)

    def combined(ref, at):
        image = for_images[0] * ref[(4, *at)]
        for j in range(1, ITERS):
            image = image + for_images[j] * ref[(4 + j, *at)]
        vector = for_vectors[0] * ref[(0, *at)]
        for j in range(1, ITERS + 1):
            vector = vector + for_vectors[j] * ref[(j, *at)]
        return image, vector

    def body(i, _):
        for row in range(0, BY, 8):
            rows = slice(row, row + 8)
            edges = combined(edges_ref, (i, rows))
            turned = [roll(value, 64, 1) for value in edges]
            for t in range(2):
                at = (i, rows, slice(t * 128, t * 128 + 128))
                values = combined(vectors_ref, at)
                if t == 0:
                    values = [jnp.where(lane < DEPTH, e, v) for e, v in zip(edges, values)]
                else:
                    values = [jnp.where(lane >= 128 - DEPTH, e, v) for e, v in zip(turned, values)]
                solution_ref[at] = values[0]
                residual_ref[at] = values[1]
        return 0

    lax.fori_loop(0, BX, body, 0)


def vmem(count):
    return [pl.BlockSpec(memory_space=VMEM)] * count


SMEM_SPEC = pl.BlockSpec(memory_space=pltpu.SMEM)


def struct(*shape):
    return jax.ShapeDtypeStruct(shape, F32)


def params(mib):
    return pltpu.CompilerParams(vmem_limit_bytes=mib << 20)


def local(right_side, wavenumber_sq, sketch_matrix):
    flip = lax.axis_index("xh").astype(jnp.int32).reshape(1)
    block = pl.pallas_call(
        prep_kernel,
        out_shape=struct(2, BX, BY, BZ),
        in_specs=[SMEM_SPEC] + vmem(2),
        out_specs=vmem(1)[0],
        compiler_params=params(8),
        name="prep",
    )(flip, right_side, wavenumber_sq)

    pairs = [(y * 2 + h, (y + (1 - 2 * h)) % 4 * 2 + h) for y in range(4) for h in range(2)]
    back = [(b, a) for a, b in pairs]
    around = [(i, (i + 1) % 4) for i in range(4)]
    inverse = [(b, a) for a, b in around]
    twin = lax.ppermute(block, "xh", [(0, 1), (1, 0)])
    outer_relay = lax.ppermute(block[:, 4:], ("y", "xh"), pairs)
    outer_twin = lax.ppermute(block[:, :4], ("y", "xh"), back)
    twin, outer_relay, outer_twin = lax.optimization_barrier((twin, outer_relay, outer_twin))
    relay = lax.ppermute(twin, ("y", "xh"), pairs)

    def pack(slots, names, *parts):
        count = len(slots)
        low, high = pl.pallas_call(
            functools.partial(pack_rows_kernel, slots, names),
            out_shape=[struct(2, count, 8, BZ)] * 2,
            in_specs=vmem(len(parts)),
            out_specs=vmem(2),
            compiler_params=params(8),
            name="pack_rows",
        )(*parts)
        above = lax.ppermute(low, ("xl", "co"), inverse)
        below = lax.ppermute(high, ("xl", "co"), around)
        return below, above

    below_1, above_1 = pack(FIRST, ("own", "twin"), block, twin)
    below_2, above_2 = pack(
        SECOND, ("relay", "outer_relay", "outer_twin"), relay, outer_relay, outer_twin
    )
    parts = (block, twin, relay, outer_relay, outer_twin, below_1, above_1, below_2, above_2)
    low, high = pl.pallas_call(
        pack_columns_kernel,
        out_shape=[struct(2, 2, 64, 128)] * 2,
        in_specs=vmem(9),
        out_specs=vmem(2),
        compiler_params=params(8),
        name="pack_columns",
    )(*parts)
    above = lax.ppermute(low, "z", inverse)
    below = lax.ppermute(high, "z", around)

    def fields(tiles):
        return [VMEM((tiles, LAYERS, ROWS, 128), F32)] * 5

    vectors, sums, edge, thin = pl.pallas_call(
        interior_kernel,
        out_shape=[struct(7, BX, BY, BZ), struct(4 * SK, 8, 128), struct(2, LAYERS, ROWS, 128), struct(SK, BX, BY, 128)],
        in_specs=[SMEM_SPEC] + vmem(10),
        out_specs=vmem(4),
        scratch_shapes=fields(2),
        compiler_params=params(20),
        cost_estimate=pl.CostEstimate(flops=30_000_000, bytes_accessed=1 << 20, transcendentals=0),
        name="interior",
    )(flip, sketch_matrix, *parts)
    edges, images = pl.pallas_call(
        edge_kernel,
        out_shape=[struct(7, BX, BY, 128), struct(128, 128)],
        in_specs=[SMEM_SPEC] + vmem(5),
        out_specs=vmem(2),
        scratch_shapes=fields(1) + [VMEM((4 * SK, 8, 128), F32)],
        compiler_params=params(12),
        name="edge",
    )(flip, edge, below, above, thin, sums)

    totals = lax.all_to_all(images, ("y", "xh", "xl", "co", "z"), 0, 0, tiled=True)
    return tuple(
        pl.pallas_call(
            final_kernel,
            out_shape=[struct(BX, BY, BZ)] * 2,
            in_specs=vmem(3),
            out_specs=vmem(2),
            compiler_params=params(8),
            name="combine",
        )(totals, vectors, edges)
    )


def solution(mesh):
    finer = Mesh(mesh.devices.reshape(4, 2, 2, 2, 4), ("y", "xh", "xl", "co", "z"))
    spec = (("y", "xh"), ("xl", "co"), "z")
    return jax.shard_map(
        local,
        mesh=finer,
        in_specs=(P(*spec), P(*spec), P(None, *spec)),
        out_specs=(P(*spec), P(*spec)),
        check_vma=False,
    )
```

```python
import functools

import jax
import jax.numpy as jnp
from jax import lax
from jax.experimental import pallas as pl
from jax.experimental.pallas import tpu as pltpu
from jax.sharding import Mesh
from jax.sharding import PartitionSpec as P


SK = 16
SWEEPS = 3
ITERS = 3
RADIUS = SWEEPS + 1
DEPTH = ITERS * RADIUS
BX, BY, BZ = 8, 32, 256
HALF = BX // 2
ROWS = 80
ROW0 = 24
LAYERS = BX + 2 * DEPTH
OWN = DEPTH
MID = LAYERS // 2
REACH = DEPTH // 2
GROUPS = (4, 4)

VMEM = pltpu.VMEM
F32 = jnp.float32
BF16 = jnp.bfloat16


def layer_of(part):
    name, idx = part
    if name == "own":
        return OWN + idx
    if name == "twin":
        return OWN + 15 - idx
    if name == "relay":
        return OWN - 1 - idx
    if name == "outer_relay":
        return idx
    return OWN + 16 + idx


def distance(layer):
    return max(0, OWN - layer, layer - (OWN + BX - 1))


ALL_PARTS = (
    [("outer_relay", i) for i in range(4)]
    + [("relay", i) for i in range(8)]
    + [("own", i) for i in range(8)]
    + [("twin", i) for i in range(8)]
    + [("outer_twin", i) for i in range(4)]
)
PART_OF = {layer_of(part): part for part in ALL_PARTS}

FIRST = (
    [("A", ("own", i)) for i in range(8)]
    + [("A", ("twin", i)) for i in range(8)]
    + [("B", ("own", i), ("own", i + 1)) for i in (0, 2, 4, 6)]
    + [("B", ("twin", i), ("twin", i + 1)) for i in (4, 6)]
)
SECOND = (
    [("A", ("relay", i)) for i in range(8)]
    + [("B", ("relay", i), ("relay", i + 1)) for i in (0, 2)]
    + [
        ("C", ("outer_relay", 1), ("outer_relay", 2)),
        ("C", ("outer_relay", 3), ("outer_twin", 0)),
        ("C", ("outer_twin", 1), ("outer_twin", 2)),
    ]
)


def lane_plan():
    plans = []
    for odd in range(2):
        plan = {}
        place, room = 0, 0
        order = list(range(1, MID))
        if odd:
            order.reverse()
        for layer in order:
            width = DEPTH - distance(layer)
            short, long = width // 2, (width + 1) // 2
            below, above = (long, short) if odd else (short, long)
            place += max(below, room) if plan else below
            room = above
            plan[layer] = (place, below, above)
        first_place, first_below, _ = plan[order[0]]
        assert 64 + first_place - place >= max(first_below, room)
        plans.append(plan)
    return plans


LANES = lane_plan()


def lanes_between(lane, start, width, period):
    return ((lane - start) & (period - 1)) < width


def roll(value, shift, axis):
    shift = shift % value.shape[axis]
    if shift == 0:
        return value
    return pltpu.roll(value, shift, axis)


def interleaving(transposed):
    rows = lax.broadcasted_iota(jnp.int32, (BZ, BZ), 1 if transposed else 0)
    cols = lax.broadcasted_iota(jnp.int32, (BZ, BZ), 0 if transposed else 1)
    source = jnp.where(cols < 128, 2 * cols, 2 * cols - (BZ - 1))
    return jnp.where(rows == source, 1.0, 0.0).astype(BF16)


def permuted(value, matrix):
    total = None
    for _ in range(3):
        piece = value.astype(BF16)
        value = value - piece.astype(F32)
        part = jnp.dot(piece, matrix, preferred_element_type=F32)
        total = part if total is None else total + part
    return total


def mirrored(flip, i, size=BX):
    return jnp.where(flip == 1, size - 1 - i, i)


def prep_kernel(flip_ref, rhs_ref, coef_ref, rhs_out, inv_out, low_out, high_out):
    flip = flip_ref[0]
    matrix = interleaving(False)
    fields = (rhs_ref[...].reshape(BX * BY, BZ), 1.0 / (6.0 + coef_ref[...].reshape(BX * BY, BZ)))
    for array, out_ref in enumerate((rhs_out, inv_out)):
        value = permuted(fields[array], matrix).reshape(BX, BY, BZ)
        for i in range(BX):
            out_ref[mirrored(flip, i)] = value[i]
        low_out[array] = out_ref[:HALF]
        high_out[array] = out_ref[HALF:]


def halves(first, second, lane):
    turned = roll(second, 64, 1)
    low = jnp.where(lane < 64, first, turned)
    high = jnp.where(lane < 64, turned, first)
    return jnp.where((lane & 63) < 16, low, roll(high, 32, 1))


def early_kernel(flip_ref, sketch, rhs_ref, sketch_out, thin_out, sums_out):
    flip = flip_ref[0]
    lane = lax.broadcasted_iota(jnp.int32, (8, 128), 1)
    matrix = interleaving(False)

    def order(s, _):
        value = permuted(sketch[s].reshape(BX * BY, BZ), matrix).reshape(BX, BY, BZ)
        for i in range(BX):
            sketch_out[s, mirrored(flip, i)] = value[i]
        for i in range(HALF):
            for row in range(0, BY, 8):
                for t in range(2):
                    cols = slice(t * 128, t * 128 + 128)
                    pair = [sketch_out[s, k, row : row + 8, cols] for k in (i, BX - 1 - i)]
                    thin_out[t, s, i, row : row + 8] = halves(*pair, lane)
        return 0

    lax.fori_loop(0, SK, order, 0)

    def field_of(j, i, row, t):
        return rhs_ref[i, row : row + 8, t * 128 : t * 128 + 128]

    def weight_of(s, i, row, t):
        return sketch_out[s, i, row : row + 8, t * 128 : t * 128 + 128]

    sketch_sums(sums_out, None, weight_of, field_of, range(1), BX, 0)


def pack_rows_kernel(slots, names, *refs):
    sources = dict(zip(names, refs))
    low_ref, high_ref = refs[len(names) :]
    sub = lax.broadcasted_iota(jnp.int32, (8, BZ), 0)
    for slot, (kind, *parts) in enumerate(slots):
        values = []
        for tiles in ((0, 1), (3, 2)):
            tile = tiles[1] if kind == "B" else tiles[0]
            values.append([sources[p][i, tile * 8 : tile * 8 + 8] for p, i in parts])
        low, high = values
        if kind == "A":
            low_ref[slot] = low[0]
            high_ref[slot] = high[0]
        else:
            low_ref[slot] = jnp.where(sub < 4, low[0], roll(low[1], 4, 0))
            high_ref[slot] = jnp.where(sub >= 4, high[0], roll(high[1], 4, 0))


def row_sources(slots):
    found = {}
    for slot, (kind, *parts) in enumerate(slots):
        for at, part in enumerate(parts):
            below, above = (0, 7) if kind == "B" else (1, 6)
            found.setdefault(part, {})[below] = (slot, at)
            found.setdefault(part, {})[above] = (slot, at)
    return found


PART_NAMES = ("own", "twin", "relay", "outer_relay", "outer_twin")
FOUND = (row_sources(FIRST), row_sources(SECOND))
N_BLOCKS = 16


class Blocks:
    def __init__(self, refs):
        pairs = [(refs[2 * i], refs[2 * i + 1]) for i in range(3)]
        outer = [(ref.at[0], ref.at[1]) for ref in refs[6:8]]
        self.sources = dict(zip(PART_NAMES, pairs + outer))
        self.below = ((refs[8], refs[9]), (refs[12], refs[13]))
        self.above = ((refs[10], refs[11]), (refs[14], refs[15]))

    def tile(self, array, part, row_tile, t):
        cols = slice(t * 128, t * 128 + 128)
        if 2 <= row_tile <= 5:
            name, idx = part
            return self.sources[name][array][idx, row_tile * 8 - 16 : row_tile * 8 - 8, cols]
        message = 0 if part in FOUND[0] else 1
        where = FOUND[message].get(part, {}).get(row_tile)
        if where is None:
            return None
        side = self.below if row_tile < 2 else self.above
        slot, rolled = where
        value = side[message][array][slot, :, cols]
        return roll(value, 4, 0) if rolled else value


def pack_columns_kernel(*refs):
    blocks = Blocks(refs)
    low_ref, high_ref = refs[N_BLOCKS:]
    lane = lax.broadcasted_iota(jnp.int32, (8, 128), 1)
    for array in range(2):
        for t in range(2):
            for row_tile in range(8):
                low = high = None
                for layer, (place, below, above) in LANES[t].items():
                    for half, at in ((0, layer), (1, LAYERS - 1 - layer)):
                        value = blocks.tile(array, PART_OF[at], row_tile, t)
                        if value is None:
                            continue
                        start = place + 64 * half
                        value = roll(value, start, 1)
                        if above:
                            mask = lanes_between(lane, start, above, 128)
                            low = value if low is None else jnp.where(mask, value, low)
                        if below:
                            mask = lanes_between(lane, start - below, below, 128)
                            high = value if high is None else jnp.where(mask, value, high)
                rows = slice(row_tile * 8, row_tile * 8 + 8)
                low_ref[array, t, rows] = roll(low, 32, 1)
                high_ref[array, t, rows] = high


def rows_of(reach):
    if reach == 0:
        return range(2, 6)
    return range(1, 7) if reach <= 8 else range(0, 8)


def over_layers(first, count, group, body):
    rest = (count - 1) % group + 1
    whole = (count - rest) // group

    def step(i, _):
        body(first + i * group, group, False)
        return 0

    if whole == 1:
        body(first, group, False)
    elif whole > 1:
        lax.fori_loop(0, whole, step, 0)
    body(first + whole * group, rest, True)


def krylov_steps(vec, inv, za, zb, mid, folded, group, lane, keep_own):
    def layers(left):
        return (OWN - left, HALF + left) if folded else (OWN - left, BX + 2 * left)

    def pass_over(source, left, store):
        def body(layer, count, last):
            for row_tile in rows_of(left):
                row = 8 + row_tile * 8
                rows = slice(row, row + 8)
                here = {
                    (l, t): source[t, layer + l, rows] for l in range(-1, count + 1) for t in range(2)
                }
                for l in range(count):
                    even, odd = here[l, 0], here[l, 1]
                    along = (odd + roll(odd, 1, 1), even + roll(even, 127, 1))
                    for t in range(2):
                        total = here[l - 1, t] + here[l + 1, t]
                        around = source[t, layer + l, row - 1 : row + 7] + source[t, layer + l, row + 1 : row + 9]
                        total = total + around + along[t]
                        value, target = store(t, layer + l, rows, here[l, t], total)
                        if target is not None:
                            target[t, layer + l, rows] = value
                            if folded and last and l == count - 1:
                                target[t, MID, rows] = roll(value, 64, 1)

        over_layers(*layers(left), group, body)

    def sweep(source, target, left, keep):
        def store(t, layer, rows, here, total):
            total = total + vec[t, layer, rows]
            if keep:
                mid[t, layer, rows] = total
            return total * inv[t, layer, rows], target

        pass_over(source, left, store)

    for step in range(ITERS):
        reach = DEPTH - step * RADIUS
        last_step = step == ITERS - 1
        sweep(za, zb, reach - 1, False)
        sweep(zb, za, reach - 2, False)
        sweep(za, zb, reach - 3, True)

        def apply(t, layer, rows, here, total):
            value = 12.0 * here - mid[t, layer, rows] - total
            vec[t, layer, rows] = value
            if last_step:
                return value, None
            return value * inv[t, layer, rows], za

        pass_over(zb, reach - 4, apply)
        keep_own(step)


def sketch_sums(sums_ref, start_ref, weight_of, field_of, fields, layers, skip):
    group = 4
    for start in range(0, SK, group):

        def body(i, carry):
            carry = list(carry)
            for row in range(0, BY, 8):
                for t in range(2):
                    values = [field_of(j, i, row, t) for j in fields]
                    for s in range(group):
                        weight = weight_of(start + s, i, row, t)
                        for j, value in enumerate(values):
                            carry[j * group + s] = carry[j * group + s] + weight * value
            return tuple(carry)

        at = [(j - skip) * SK + start + s for j in fields for s in range(group)]
        if start_ref is None:
            zero = jnp.zeros((8, 128), F32)
            init = (zero,) * len(at)
        else:
            init = tuple(start_ref[k] for k in at)
        for k, value in zip(at, lax.fori_loop(0, layers, body, init)):
            sums_ref[k] = value


def own_rows(source, layers, store):
    def body(i, _):
        for row in range(0, BY, 8):
            for t in range(2):
                store(i, row, t, source[t, OWN + i, ROW0 + row : ROW0 + row + 8])
        return 0

    lax.fori_loop(0, layers, body, 0)


def interior_kernel(sketch, *refs):
    blocks = Blocks(refs[:N_BLOCKS])
    vectors_ref, sums_ref, edge_ref, vec, inv, za, zb, mid = refs[N_BLOCKS:]
    lane = lax.broadcasted_iota(jnp.int32, (8, 128), 1)

    for layer in range(MID):
        pair = [PART_OF[layer], PART_OF[LAYERS - 1 - layer]]
        for row_tile in range(8):
            if blocks.tile(0, pair[0], row_tile, 0) is None:
                continue
            rows = slice(8 + row_tile * 8, 16 + row_tile * 8)
            for t in range(2):
                values = [[blocks.tile(array, part, row_tile, t) for part in pair] for array in range(2)]
                for at, value, scale in zip((layer, LAYERS - 1 - layer), *values):
                    vec[t, at, rows] = value
                    inv[t, at, rows] = scale
                    za[t, at, rows] = value * scale
                for array in range(2):
                    edge_ref[array, t, layer, rows] = halves(*values[array], lane)

    def keeper(place):
        def store(i, row, t, value):
            vectors_ref[place, i, row : row + 8, t * 128 : t * 128 + 128] = value

        return store

    def keep_own(step):
        own_rows(vec, BX, keeper(1 + step))
        own_rows(zb, BX, keeper(4 + step))

    own_rows(vec, BX, keeper(0))
    krylov_steps(vec, inv, za, zb, mid, False, GROUPS[0], lane, keep_own)
    inside = (lane >= REACH) & (lane < 128 - REACH)

    def field_of(j, i, row, t):
        return jnp.where(inside, vectors_ref[j, i, row : row + 8, t * 128 : t * 128 + 128], 0.0)

    def weight_of(s, i, row, t):
        return sketch[s, i, row : row + 8, t * 128 : t * 128 + 128]

    sketch_sums(sums_ref, None, weight_of, field_of, range(1, 4), BX, 1)


def edge_kernel(edge_ref, below_ref, above_ref, thin, first_ref, before_ref, vectors_ref, images_ref, vec, inv, za, zb, mid, sums):
    lane = lax.broadcasted_iota(jnp.int32, (8, 128), 1)
    half = lane & 63

    for t in range(2):
        for row in range(ROW0, ROW0 + BY, 8):
            rows = slice(row, row + 8)
            za[t, 0, rows] = edge_ref[0, t, 0, rows] * edge_ref[1, t, 0, rows]
        for layer, (place, below, above) in LANES[t].items():
            mask = lanes_between(lane, place - below, below, 64)
            for row_tile in rows_of(DEPTH) if distance(layer) <= 3 else rows_of(8):
                at = slice(8 + row_tile * 8, 16 + row_tile * 8)
                rows = slice(row_tile * 8, row_tile * 8 + 8)
                values = []
                for array in range(2):
                    halo = jnp.where(mask, below_ref[array, t, rows], above_ref[array, t, rows])
                    values.append(jnp.where(half < 32, edge_ref[array, t, layer, at], roll(halo, -place, 1)))
                vec[t, layer, at] = values[0]
                inv[t, layer, at] = values[1]
                product = values[0] * values[1]
                za[t, layer, at] = product
                if layer == MID - 1:
                    za[t, MID, at] = roll(product, 64, 1)

    def keeper(place):
        def store(i, row, t, value):
            vectors_ref[place, t, i, row : row + 8] = value

        return store

    def keep_own(step):
        own_rows(vec, HALF, keeper(1 + step))
        own_rows(zb, HALF, keeper(4 + step))

    own_rows(vec, HALF, keeper(0))
    krylov_steps(vec, inv, za, zb, mid, True, GROUPS[1], lane, keep_own)
    inside = (half < REACH) | ((half >= 32 - REACH) & (half < 32))

    def field_of(j, i, row, t):
        return jnp.where(inside, vectors_ref[j, t, i, row : row + 8], 0.0)

    def weight_of(s, i, row, t):
        return thin[t, s, i, row : row + 8]

    sketch_sums(sums, before_ref, weight_of, field_of, range(1, 4), HALF, 1)
    lanes = lax.broadcasted_iota(jnp.int32, (1, 128), 1)
    image = jnp.zeros((1, 128), F32)
    for k in range(4 * SK):
        value = first_ref[k] if k < SK else sums[k - SK]
        value = jnp.sum(jnp.sum(value, axis=0, keepdims=True), axis=1, keepdims=True)
        image = jnp.where(lanes == k, value, image)
    images_ref[...] = jnp.broadcast_to(image, images_ref.shape)


def dot(left, right):
    return jnp.sum(left * right, axis=0, keepdims=True)


def small_solve(totals):
    row = lax.broadcasted_iota(jnp.int32, (4 * SK, 128), 0)
    col = lax.broadcasted_iota(jnp.int32, (4 * SK, 128), 1)
    wide = jnp.where(row == col, jnp.broadcast_to(totals, (4 * SK, 128)), 0.0)
    spread = jnp.broadcast_to(jnp.sum(wide, axis=1, keepdims=True), (4 * SK, 128))
    sketches = [spread[j * SK : (j + 1) * SK] for j in range(4)]
    zero = jnp.zeros((1, 128), F32)
    beta = jnp.sqrt(dot(sketches[0], sketches[0]))
    basis = [[1.0 / beta, zero, zero, zero]]
    images = [sketches[0] / beta]
    hessen = [[zero] * ITERS for _ in range(ITERS + 1)]
    for j in range(ITERS):
        combo = [zero] + [basis[j][i] for i in range(3)]
        image = combo[1] * sketches[1]
        for i in range(1, j + 1):
            image = image + combo[i + 1] * sketches[i + 1]
        weights = [dot(member, image) for member in images]
        rest = image
        for i in range(j + 1):
            rest = rest - weights[i] * images[i]
            combo = [combo[k] - weights[i] * basis[i][k] for k in range(4)]
            hessen[i][j] = weights[i]
        length = jnp.sqrt(dot(rest, rest))
        hessen[j + 1][j] = length
        basis.append([entry / length for entry in combo])
        images.append(rest / length)
    target = [beta, zero, zero, zero]

    def inner(left, right):
        total = left[0] * right[0]
        for a, b in zip(left[1:], right[1:]):
            total = total + a * b
        return total

    members = []
    upper = [[None] * ITERS for _ in range(ITERS)]
    for j in range(ITERS):
        column = [hessen[i][j] for i in range(ITERS + 1)]
        for i in range(j):
            factor = inner(members[i], column)
            upper[i][j] = factor
            column = [c - factor * m for c, m in zip(column, members[i])]
        diag = jnp.sqrt(inner(column, column))
        upper[j][j] = diag
        members.append([c / diag for c in column])
    coeffs = [None] * ITERS
    for j in reversed(range(ITERS)):
        accum = inner(members[j], target)
        for i in range(j + 1, ITERS):
            accum = accum - upper[j][i] * coeffs[i]
        coeffs[j] = accum / upper[j][j]
    leftover = []
    for i in range(ITERS + 1):
        total = hessen[i][0] * coeffs[0]
        for j in range(1, ITERS):
            total = total + hessen[i][j] * coeffs[j]
        leftover.append(target[i] - total)
    for_images = []
    for i in range(ITERS):
        total = coeffs[0] * basis[0][i]
        for j in range(1, ITERS):
            total = total + coeffs[j] * basis[j][i]
        for_images.append(total)
    for_vectors = []
    for i in range(ITERS + 1):
        total = leftover[0] * basis[0][i]
        for j in range(1, ITERS + 1):
            total = total + leftover[j] * basis[j][i]
        for_vectors.append(total)
    return for_images, for_vectors


def final_kernel(flip_ref, sums_ref, vectors_ref, edges_ref, solution_ref, residual_ref, merged):
    flip = flip_ref[0]
    totals = jnp.sum(sums_ref[...], axis=0, keepdims=True)
    for_images, for_vectors = small_solve(totals)
    for_images = [jnp.broadcast_to(w, (8, 128)) for w in for_images]
    for_vectors = [jnp.broadcast_to(w, (8, 128)) for w in for_vectors]
    lane = lax.broadcasted_iota(jnp.int32, (8, 128), 1)

    def combined(load):
        image = for_images[0] * load(4)
        for j in range(1, ITERS):
            image = image + for_images[j] * load(4 + j)
        vector = for_vectors[0] * load(0)
        for j in range(1, ITERS + 1):
            vector = vector + for_vectors[j] * load(j)
        return image, vector

    def body(i, _):
        for row in range(0, BY, 8):
            rows = slice(row, row + 8)
            for t in range(2):
                cols = slice(t * 128, t * 128 + 128)
                edges = combined(lambda j: edges_ref[j, t, i, rows])
                for layer, low, high in ((i, 0, 96), (BX - 1 - i, 64, 32)):
                    values = combined(lambda j: vectors_ref[j, layer, rows, cols])
                    for out, (edge, value) in enumerate(zip(edges, values)):
                        value = jnp.where(lane < REACH, roll(edge, low, 1), value)
                        value = jnp.where(lane >= 128 - REACH, roll(edge, high, 1), value)
                        merged[out, mirrored(flip, layer), rows, cols] = value
        return 0

    lax.fori_loop(0, HALF, body, 0)
    matrix = interleaving(True)
    for out, out_ref in enumerate((solution_ref, residual_ref)):
        out_ref[...] = permuted(merged[out].reshape(BX * BY, BZ), matrix).reshape(BX, BY, BZ)


def vmem(count):
    return [pl.BlockSpec(memory_space=VMEM)] * count


SMEM_SPEC = pl.BlockSpec(memory_space=pltpu.SMEM)


def struct(*shape):
    return jax.ShapeDtypeStruct(shape, F32)


def params(mib):
    return pltpu.CompilerParams(vmem_limit_bytes=mib << 20)


def cost(flops):
    return pl.CostEstimate(flops=flops, bytes_accessed=1 << 20, transcendentals=0)


def fields(layers):
    return [VMEM((2, layers, ROWS, 128), F32)] * 5


def local(right_side, wavenumber_sq, sketch_matrix):
    flip = lax.axis_index("xh").astype(jnp.int32).reshape(1)
    rhs, inv, low_half, high_half = pl.pallas_call(
        prep_kernel,
        out_shape=[struct(BX, BY, BZ)] * 2 + [struct(2, HALF, BY, BZ)] * 2,
        in_specs=[SMEM_SPEC] + vmem(2),
        out_specs=vmem(4),
        compiler_params=params(8),
        name="prep",
    )(flip, right_side, wavenumber_sq)

    pairs = [(y * 2 + h, (y + (1 - 2 * h)) % 4 * 2 + h) for y in range(4) for h in range(2)]
    back = [(b, a) for a, b in pairs]
    around = [(i, (i + 1) % 4) for i in range(4)]
    inverse = [(b, a) for a, b in around]

    def pack(slots, names, *parts):
        low, high = pl.pallas_call(
            functools.partial(pack_rows_kernel, slots, names),
            out_shape=[struct(len(slots), 8, BZ)] * 2,
            in_specs=vmem(len(parts)),
            out_specs=vmem(2),
            compiler_params=params(8),
            name="pack_rows",
        )(*parts)
        above = lax.ppermute(low, ("xl", "co"), inverse)
        below = lax.ppermute(high, ("xl", "co"), around)
        return below, above

    own = (rhs, inv)
    twin = [lax.ppermute(field, "xh", [(0, 1), (1, 0)]) for field in own]
    outer_relay = lax.ppermute(high_half, ("y", "xh"), pairs)
    outer_twin = lax.ppermute(low_half, ("y", "xh"), back)
    sketch, thin, first_sums = pl.pallas_call(
        early_kernel,
        out_shape=[struct(SK, BX, BY, BZ), struct(2, SK, HALF, BY, 128), struct(SK, 8, 128)],
        in_specs=[SMEM_SPEC] + vmem(2),
        out_specs=vmem(3),
        compiler_params=params(16),
        cost_estimate=cost(20_000_000),
        name="early",
    )(flip, sketch_matrix, rhs)
    relay, first, second = [], [], []
    for field, other in zip(own, twin):
        relay.append(lax.ppermute(other, ("y", "xh"), pairs))
        first.append(pack(FIRST, ("own", "twin"), field, other))
    for array in range(2):
        second.append(
            pack(
                SECOND,
                ("relay", "outer_relay", "outer_twin"),
                relay[array],
                outer_relay[array],
                outer_twin[array],
            )
        )
    parts = (
        *own, *twin, *relay, outer_relay, outer_twin,
        first[0][0], first[1][0], first[0][1], first[1][1],
        second[0][0], second[1][0], second[0][1], second[1][1],
    )
    low, high = pl.pallas_call(
        pack_columns_kernel,
        out_shape=[struct(2, 2, 64, 128)] * 2,
        in_specs=vmem(N_BLOCKS),
        out_specs=vmem(2),
        compiler_params=params(8),
        name="pack_columns",
    )(*parts)
    above = lax.ppermute(low, "z", inverse)
    below = lax.ppermute(high, "z", around)
    vectors, sums, edge = pl.pallas_call(
        interior_kernel,
        out_shape=[struct(7, BX, BY, BZ), struct(3 * SK, 8, 128), struct(2, 2, MID, ROWS, 128)],
        in_specs=vmem(1 + N_BLOCKS),
        out_specs=vmem(3),
        scratch_shapes=fields(LAYERS),
        compiler_params=params(20),
        cost_estimate=cost(30_000_000),
        name="interior",
    )(sketch, *parts)
    edges, images = pl.pallas_call(
        edge_kernel,
        out_shape=[struct(7, 2, HALF, BY, 128), struct(128, 128)],
        in_specs=vmem(6),
        out_specs=vmem(2),
        scratch_shapes=fields(MID + 1) + [VMEM((3 * SK, 8, 128), F32)],
        compiler_params=params(12),
        name="edge",
    )(edge, below, above, thin, first_sums, sums)

    totals = lax.all_to_all(images, ("y", "xh", "xl", "co", "z"), 0, 0, tiled=True)
    return tuple(
        pl.pallas_call(
            final_kernel,
            out_shape=[struct(BX, BY, BZ)] * 2,
            in_specs=[SMEM_SPEC] + vmem(3),
            out_specs=vmem(2),
            scratch_shapes=[VMEM((2, BX, BY, BZ), F32)],
            compiler_params=params(8),
            name="combine",
        )(flip, totals, vectors, edges)
    )


def solution(mesh):
    finer = Mesh(mesh.devices.reshape(4, 2, 2, 2, 4), ("y", "xh", "xl", "co", "z"))
    spec = (("y", "xh"), ("xl", "co"), "z")
    return jax.shard_map(
        local,
        mesh=finer,
        in_specs=(P(*spec), P(*spec), P(None, *spec)),
        out_specs=(P(*spec), P(*spec)),
        check_vma=False,
    )
```

```python
import functools

import jax
import jax.numpy as jnp
from jax import lax
from jax.experimental import pallas as pl
from jax.experimental.pallas import tpu as pltpu
from jax.sharding import Mesh
from jax.sharding import PartitionSpec as P


SK = 16
SWEEPS = 3
ITERS = 3
RADIUS = SWEEPS + 1
DEPTH = ITERS * RADIUS
BX, BY, BZ = 8, 32, 256
HALF = BX // 2
ROWS = 80
ROW0 = 24
LAYERS = BX + 2 * DEPTH
OWN = DEPTH
MID = LAYERS // 2
REACH = DEPTH // 2
GROUPS = (4, 4)

VMEM = pltpu.VMEM
F32 = jnp.float32
BF16 = jnp.bfloat16


def layer_of(part):
    name, idx = part
    if name == "own":
        return OWN + idx
    if name == "twin":
        return OWN + 15 - idx
    if name == "relay":
        return OWN - 1 - idx
    if name == "outer_relay":
        return idx
    return OWN + 16 + idx


def distance(layer):
    return max(0, OWN - layer, layer - (OWN + BX - 1))


ALL_PARTS = (
    [("outer_relay", i) for i in range(4)]
    + [("relay", i) for i in range(8)]
    + [("own", i) for i in range(8)]
    + [("twin", i) for i in range(8)]
    + [("outer_twin", i) for i in range(4)]
)
PART_OF = {layer_of(part): part for part in ALL_PARTS}

FIRST = (
    [("A", ("own", i)) for i in range(8)]
    + [("A", ("twin", i)) for i in range(8)]
    + [("B", ("own", i), ("own", i + 1)) for i in (0, 2, 4, 6)]
    + [("B", ("twin", i), ("twin", i + 1)) for i in (4, 6)]
)
SECOND = (
    [("A", ("relay", i)) for i in range(8)]
    + [("B", ("relay", i), ("relay", i + 1)) for i in (0, 2)]
    + [
        ("C", ("outer_relay", 1), ("outer_relay", 2)),
        ("C", ("outer_relay", 3), ("outer_twin", 0)),
        ("C", ("outer_twin", 1), ("outer_twin", 2)),
    ]
)


def lane_plan():
    plans = []
    for odd in range(2):
        plan = {}
        place, room = 0, 0
        order = list(range(1, MID))
        if odd:
            order.reverse()
        for layer in order:
            width = DEPTH - distance(layer)
            short, long = width // 2, (width + 1) // 2
            below, above = (long, short) if odd else (short, long)
            place += max(below, room) if plan else below
            room = above
            plan[layer] = (place, below, above)
        first_place, first_below, _ = plan[order[0]]
        assert 64 + first_place - place >= max(first_below, room)
        plans.append(plan)
    return plans


LANES = lane_plan()


def lanes_between(lane, start, width, period):
    return ((lane - start) & (period - 1)) < width


def roll(value, shift, axis):
    shift = shift % value.shape[axis]
    if shift == 0:
        return value
    return pltpu.roll(value, shift, axis)


def interleaving(transposed):
    rows = lax.broadcasted_iota(jnp.int32, (BZ, BZ), 1 if transposed else 0)
    cols = lax.broadcasted_iota(jnp.int32, (BZ, BZ), 0 if transposed else 1)
    source = jnp.where(cols < 128, 2 * cols, 2 * cols - (BZ - 1))
    return jnp.where(rows == source, 1.0, 0.0).astype(BF16)


def permuted(value, matrix):
    total = None
    for _ in range(3):
        piece = value.astype(BF16)
        value = value - piece.astype(F32)
        part = jnp.dot(piece, matrix, preferred_element_type=F32)
        total = part if total is None else total + part
    return total


def mirrored(flip, i, size=BX):
    return jnp.where(flip == 1, size - 1 - i, i)


def prep_kernel(flip_ref, rhs_ref, coef_ref, rhs_out, inv_out, low_out, high_out):
    flip = flip_ref[0]
    matrix = interleaving(False)
    fields = (rhs_ref[...].reshape(BX * BY, BZ), 1.0 / (6.0 + coef_ref[...].reshape(BX * BY, BZ)))
    for array, out_ref in enumerate((rhs_out, inv_out)):
        value = permuted(fields[array], matrix).reshape(BX, BY, BZ)
        for i in range(BX):
            out_ref[mirrored(flip, i)] = value[i]
        low_out[array] = out_ref[:HALF]
        high_out[array] = out_ref[HALF:]


def halves(first, second, lane):
    turned = roll(second, 64, 1)
    low = jnp.where(lane < 64, first, turned)
    high = jnp.where(lane < 64, turned, first)
    return jnp.where((lane & 63) < 16, low, roll(high, 32, 1))


def first_kernel(rhs_ref, sketch, sums_out):
    def field_of(j, i, row, cols):
        return rhs_ref[i, row : row + 8, cols]

    sketch_sums(sums_out, sketch, field_of, range(1))


def pack_rows_kernel(slots, names, *refs):
    sources = dict(zip(names, refs))
    low_ref, high_ref = refs[len(names) :]
    sub = lax.broadcasted_iota(jnp.int32, (8, BZ), 0)
    for slot, (kind, *parts) in enumerate(slots):
        values = []
        for tiles in ((0, 1), (3, 2)):
            tile = tiles[1] if kind == "B" else tiles[0]
            values.append([sources[p][i, tile * 8 : tile * 8 + 8] for p, i in parts])
        low, high = values
        if kind == "A":
            low_ref[slot] = low[0]
            high_ref[slot] = high[0]
        else:
            low_ref[slot] = jnp.where(sub < 4, low[0], roll(low[1], 4, 0))
            high_ref[slot] = jnp.where(sub >= 4, high[0], roll(high[1], 4, 0))


def row_sources(slots):
    found = {}
    for slot, (kind, *parts) in enumerate(slots):
        for at, part in enumerate(parts):
            below, above = (0, 7) if kind == "B" else (1, 6)
            found.setdefault(part, {})[below] = (slot, at)
            found.setdefault(part, {})[above] = (slot, at)
    return found


PART_NAMES = ("own", "twin", "relay", "outer_relay", "outer_twin")
FOUND = (row_sources(FIRST), row_sources(SECOND))
N_BLOCKS = 16


class Blocks:
    def __init__(self, refs):
        pairs = [(refs[2 * i], refs[2 * i + 1]) for i in range(3)]
        outer = [(ref.at[0], ref.at[1]) for ref in refs[6:8]]
        self.sources = dict(zip(PART_NAMES, pairs + outer))
        self.below = ((refs[8], refs[9]), (refs[12], refs[13]))
        self.above = ((refs[10], refs[11]), (refs[14], refs[15]))

    def tile(self, array, part, row_tile, t):
        cols = slice(t * 128, t * 128 + 128)
        if 2 <= row_tile <= 5:
            name, idx = part
            return self.sources[name][array][idx, row_tile * 8 - 16 : row_tile * 8 - 8, cols]
        message = 0 if part in FOUND[0] else 1
        where = FOUND[message].get(part, {}).get(row_tile)
        if where is None:
            return None
        side = self.below if row_tile < 2 else self.above
        slot, rolled = where
        value = side[message][array][slot, :, cols]
        return roll(value, 4, 0) if rolled else value


def pack_columns_kernel(*refs):
    blocks = Blocks(refs)
    low_ref, high_ref = refs[N_BLOCKS:]
    lane = lax.broadcasted_iota(jnp.int32, (8, 128), 1)
    for array in range(2):
        for t in range(2):
            for row_tile in range(8):
                low = high = None
                for layer, (place, below, above) in LANES[t].items():
                    for half, at in ((0, layer), (1, LAYERS - 1 - layer)):
                        value = blocks.tile(array, PART_OF[at], row_tile, t)
                        if value is None:
                            continue
                        start = place + 64 * half
                        value = roll(value, start, 1)
                        if above:
                            mask = lanes_between(lane, start, above, 128)
                            low = value if low is None else jnp.where(mask, value, low)
                        if below:
                            mask = lanes_between(lane, start - below, below, 128)
                            high = value if high is None else jnp.where(mask, value, high)
                rows = slice(row_tile * 8, row_tile * 8 + 8)
                low_ref[array, t, rows] = roll(low, 32, 1)
                high_ref[array, t, rows] = high


def rows_of(reach):
    if reach == 0:
        return range(2, 6)
    return range(1, 7) if reach <= 8 else range(0, 8)


def over_layers(first, count, group, body):
    rest = (count - 1) % group + 1
    whole = (count - rest) // group

    def step(i, _):
        body(first + i * group, group, False)
        return 0

    if whole == 1:
        body(first, group, False)
    elif whole > 1:
        lax.fori_loop(0, whole, step, 0)
    body(first + whole * group, rest, True)


def krylov_steps(vec, inv, za, zb, mid, folded, group, keep_own):
    def layers(left):
        return (OWN - left, HALF + left) if folded else (OWN - left, BX + 2 * left)

    def pass_over(source, left, store):
        def body(layer, count, last):
            for row_tile in rows_of(left):
                row = 8 + row_tile * 8
                rows = slice(row, row + 8)
                here = {
                    (l, t): source[t, layer + l, rows] for l in range(-1, count + 1) for t in range(2)
                }
                for l in range(count):
                    even, odd = here[l, 0], here[l, 1]
                    along = (odd + roll(odd, 1, 1), even + roll(even, 127, 1))
                    for t in range(2):
                        total = here[l - 1, t] + here[l + 1, t]
                        around = source[t, layer + l, row - 1 : row + 7] + source[t, layer + l, row + 1 : row + 9]
                        total = total + around + along[t]
                        value, target = store(t, layer + l, rows, here[l, t], total)
                        if target is not None:
                            target[t, layer + l, rows] = value
                            if folded and last and l == count - 1:
                                target[t, MID, rows] = roll(value, 64, 1)

        over_layers(*layers(left), group, body)

    def sweep(source, target, left, keep):
        def store(t, layer, rows, here, total):
            total = total + vec[t, layer, rows]
            if keep:
                mid[t, layer, rows] = total
            return total * inv[t, layer, rows], target

        pass_over(source, left, store)

    for step in range(ITERS):
        reach = DEPTH - step * RADIUS
        last_step = step == ITERS - 1
        sweep(za, zb, reach - 1, False)
        sweep(zb, za, reach - 2, False)
        sweep(za, zb, reach - 3, True)

        def apply(t, layer, rows, here, total):
            value = 12.0 * here - mid[t, layer, rows] - total
            vec[t, layer, rows] = value
            if last_step:
                return value, None
            return value * inv[t, layer, rows], za

        pass_over(zb, reach - 4, apply)
        keep_own(step)


def sketch_sums(sums_ref, sketch, field_of, fields):
    group = 4
    for start in range(0, SK, group):

        def body(i, carry):
            carry = list(carry)
            for row in range(0, BY, 8):
                for t in range(2):
                    cols = slice(t * 128, t * 128 + 128)
                    values = [field_of(j, i, row, cols) for j in fields]
                    for s in range(group):
                        weight = sketch[start + s, i, row : row + 8, cols]
                        for j, value in enumerate(values):
                            carry[j * group + s] = carry[j * group + s] + weight * value
            return tuple(carry)

        init = (jnp.zeros((8, 128), F32),) * (len(fields) * group)
        for k, value in enumerate(lax.fori_loop(0, BX, body, init)):
            sums_ref[k // group * SK + start + k % group] = value


def own_rows(source, layers, store):
    def body(i, _):
        for row in range(0, BY, 8):
            for t in range(2):
                store(i, row, t, source[t, OWN + i, ROW0 + row : ROW0 + row + 8])
        return 0

    lax.fori_loop(0, layers, body, 0)


def interior_kernel(*refs):
    blocks = Blocks(refs[:N_BLOCKS])
    vectors_ref, edge_ref, vec, inv, za, zb, mid = refs[N_BLOCKS:]
    lane = lax.broadcasted_iota(jnp.int32, (8, 128), 1)

    for layer in range(MID):
        pair = [PART_OF[layer], PART_OF[LAYERS - 1 - layer]]
        for row_tile in range(8):
            if blocks.tile(0, pair[0], row_tile, 0) is None:
                continue
            rows = slice(8 + row_tile * 8, 16 + row_tile * 8)
            for t in range(2):
                values = [[blocks.tile(array, part, row_tile, t) for part in pair] for array in range(2)]
                for at, value, scale in zip((layer, LAYERS - 1 - layer), *values):
                    vec[t, at, rows] = value
                    inv[t, at, rows] = scale
                    za[t, at, rows] = value * scale
                for array in range(2):
                    edge_ref[array, t, layer, rows] = halves(*values[array], lane)

    def keeper(place):
        def store(i, row, t, value):
            vectors_ref[place, i, row : row + 8, t * 128 : t * 128 + 128] = value

        return store

    def keep_own(step):
        own_rows(vec, BX, keeper(step))
        own_rows(zb, BX, keeper(ITERS + step))

    krylov_steps(vec, inv, za, zb, mid, False, GROUPS[0], keep_own)


def with_edges(edge, lane, values):
    for value, low, high in zip(values, (0, 64), (96, 32)):
        value = jnp.where(lane < REACH, roll(edge, low, 1), value)
        yield jnp.where(lane >= 128 - REACH, roll(edge, high, 1), value)


def edge_kernel(
    flip_ref, edge_ref, below_ref, above_ref, sketch, first_ref, main_ref,
    vectors_ref, directions_ref, images_ref, vec, inv, za, zb, mid, sums, merged,
):
    lane = lax.broadcasted_iota(jnp.int32, (8, 128), 1)
    half = lane & 63

    for t in range(2):
        for row in range(ROW0, ROW0 + BY, 8):
            rows = slice(row, row + 8)
            za[t, 0, rows] = edge_ref[0, t, 0, rows] * edge_ref[1, t, 0, rows]
        for layer, (place, below, above) in LANES[t].items():
            mask = lanes_between(lane, place - below, below, 64)
            for row_tile in rows_of(DEPTH) if distance(layer) <= 3 else rows_of(8):
                at = slice(8 + row_tile * 8, 16 + row_tile * 8)
                rows = slice(row_tile * 8, row_tile * 8 + 8)
                values = []
                for array in range(2):
                    halo = jnp.where(mask, below_ref[array, t, rows], above_ref[array, t, rows])
                    values.append(jnp.where(half < 32, edge_ref[array, t, layer, at], roll(halo, -place, 1)))
                vec[t, layer, at] = values[0]
                inv[t, layer, at] = values[1]
                product = values[0] * values[1]
                za[t, layer, at] = product
                if layer == MID - 1:
                    za[t, MID, at] = roll(product, 64, 1)

    def keep_own(step):
        def merge(i, row, t, value):
            cols = slice(t * 128, t * 128 + 128)
            at = (i, BX - 1 - i)
            main = [main_ref[step, k, row : row + 8, cols] for k in at]
            for k, out in zip(at, with_edges(value, lane, main)):
                merged[step, k, row : row + 8, cols] = out

        def keep(i, row, t, value):
            directions_ref[step, t, i, row : row + 8] = value

        own_rows(vec, HALF, merge)
        own_rows(zb, HALF, keep)

    krylov_steps(vec, inv, za, zb, mid, True, GROUPS[1], keep_own)
    flip = flip_ref[0]
    matrix = interleaving(True)
    for j in range(ITERS):
        value = permuted(merged[j].reshape(BX * BY, BZ), matrix).reshape(BX, BY, BZ)
        for i in range(BX):
            vectors_ref[j, mirrored(flip, i)] = value[i]

    def field_of(j, i, row, cols):
        return vectors_ref[j, i, row : row + 8, cols]

    sketch_sums(sums, sketch, field_of, range(ITERS))
    lanes = lax.broadcasted_iota(jnp.int32, (1, 128), 1)
    image = jnp.zeros((1, 128), F32)
    for k in range(4 * SK):
        value = first_ref[k] if k < SK else sums[k - SK]
        value = jnp.sum(jnp.sum(value, axis=0, keepdims=True), axis=1, keepdims=True)
        image = jnp.where(lanes == k, value, image)
    images_ref[...] = jnp.broadcast_to(image, images_ref.shape)


def dot(left, right):
    return jnp.sum(left * right, axis=0, keepdims=True)


def small_solve(totals):
    row = lax.broadcasted_iota(jnp.int32, (4 * SK, 128), 0)
    col = lax.broadcasted_iota(jnp.int32, (4 * SK, 128), 1)
    wide = jnp.where(row == col, jnp.broadcast_to(totals, (4 * SK, 128)), 0.0)
    spread = jnp.broadcast_to(jnp.sum(wide, axis=1, keepdims=True), (4 * SK, 128))
    sketches = [spread[j * SK : (j + 1) * SK] for j in range(4)]
    zero = jnp.zeros((1, 128), F32)
    beta = jnp.sqrt(dot(sketches[0], sketches[0]))
    basis = [[1.0 / beta, zero, zero, zero]]
    images = [sketches[0] / beta]
    hessen = [[zero] * ITERS for _ in range(ITERS + 1)]
    for j in range(ITERS):
        combo = [zero] + [basis[j][i] for i in range(3)]
        image = combo[1] * sketches[1]
        for i in range(1, j + 1):
            image = image + combo[i + 1] * sketches[i + 1]
        weights = [dot(member, image) for member in images]
        rest = image
        for i in range(j + 1):
            rest = rest - weights[i] * images[i]
            combo = [combo[k] - weights[i] * basis[i][k] for k in range(4)]
            hessen[i][j] = weights[i]
        length = jnp.sqrt(dot(rest, rest))
        hessen[j + 1][j] = length
        basis.append([entry / length for entry in combo])
        images.append(rest / length)
    target = [beta, zero, zero, zero]

    def inner(left, right):
        total = left[0] * right[0]
        for a, b in zip(left[1:], right[1:]):
            total = total + a * b
        return total

    members = []
    upper = [[None] * ITERS for _ in range(ITERS)]
    for j in range(ITERS):
        column = [hessen[i][j] for i in range(ITERS + 1)]
        for i in range(j):
            factor = inner(members[i], column)
            upper[i][j] = factor
            column = [c - factor * m for c, m in zip(column, members[i])]
        diag = jnp.sqrt(inner(column, column))
        upper[j][j] = diag
        members.append([c / diag for c in column])
    coeffs = [None] * ITERS
    for j in reversed(range(ITERS)):
        accum = inner(members[j], target)
        for i in range(j + 1, ITERS):
            accum = accum - upper[j][i] * coeffs[i]
        coeffs[j] = accum / upper[j][j]
    leftover = []
    for i in range(ITERS + 1):
        total = hessen[i][0] * coeffs[0]
        for j in range(1, ITERS):
            total = total + hessen[i][j] * coeffs[j]
        leftover.append(target[i] - total)
    for_images = []
    for i in range(ITERS):
        total = coeffs[0] * basis[0][i]
        for j in range(1, ITERS):
            total = total + coeffs[j] * basis[j][i]
        for_images.append(total)
    for_vectors = []
    for i in range(ITERS + 1):
        total = leftover[0] * basis[0][i]
        for j in range(1, ITERS + 1):
            total = total + leftover[j] * basis[j][i]
        for_vectors.append(total)
    return for_images, for_vectors


def final_kernel(flip_ref, sums_ref, rhs_ref, vectors_ref, main_ref, edges_ref, solution_ref, residual_ref, merged):
    flip = flip_ref[0]
    totals = jnp.sum(sums_ref[...], axis=0, keepdims=True)
    for_images, for_vectors = small_solve(totals)
    for_images = [jnp.broadcast_to(w, (8, 128)) for w in for_images]
    for_vectors = [jnp.broadcast_to(w, (8, 128)) for w in for_vectors]
    lane = lax.broadcasted_iota(jnp.int32, (8, 128), 1)

    def image(load):
        total = for_images[0] * load(0)
        for j in range(1, ITERS):
            total = total + for_images[j] * load(j)
        return total

    def body(i, _):
        at = (i, BX - 1 - i)
        for row in range(0, BY, 8):
            rows = slice(row, row + 8)
            for t in range(2):
                cols = slice(t * 128, t * 128 + 128)
                edge = image(lambda j: edges_ref[j, t, i, rows])
                main = [image(lambda j: main_ref[ITERS + j, k, rows, cols]) for k in at]
                for k, value in zip(at, with_edges(edge, lane, main)):
                    merged[mirrored(flip, k), rows, cols] = value
                for k in at:
                    total = for_vectors[0] * rhs_ref[k, rows, cols]
                    for j in range(ITERS):
                        total = total + for_vectors[j + 1] * vectors_ref[j, k, rows, cols]
                    residual_ref[k, rows, cols] = total
        return 0

    lax.fori_loop(0, HALF, body, 0)
    value = permuted(merged[...].reshape(BX * BY, BZ), interleaving(True))
    solution_ref[...] = value.reshape(BX, BY, BZ)


def vmem(count):
    return [pl.BlockSpec(memory_space=VMEM)] * count


SMEM_SPEC = pl.BlockSpec(memory_space=pltpu.SMEM)


def struct(*shape):
    return jax.ShapeDtypeStruct(shape, F32)


def params(mib):
    return pltpu.CompilerParams(vmem_limit_bytes=mib << 20)


def cost(flops):
    return pl.CostEstimate(flops=flops, bytes_accessed=1 << 20, transcendentals=0)


def fields(layers):
    return [VMEM((2, layers, ROWS, 128), F32)] * 5


def local(right_side, wavenumber_sq, sketch_matrix):
    flip = lax.axis_index("xh").astype(jnp.int32).reshape(1)
    rhs, inv, low_half, high_half = pl.pallas_call(
        prep_kernel,
        out_shape=[struct(BX, BY, BZ)] * 2 + [struct(2, HALF, BY, BZ)] * 2,
        in_specs=[SMEM_SPEC] + vmem(2),
        out_specs=vmem(4),
        compiler_params=params(8),
        name="prep",
    )(flip, right_side, wavenumber_sq)

    pairs = [(y * 2 + h, (y + (1 - 2 * h)) % 4 * 2 + h) for y in range(4) for h in range(2)]
    back = [(b, a) for a, b in pairs]
    around = [(i, (i + 1) % 4) for i in range(4)]
    inverse = [(b, a) for a, b in around]

    def pack(slots, names, *parts):
        low, high = pl.pallas_call(
            functools.partial(pack_rows_kernel, slots, names),
            out_shape=[struct(len(slots), 8, BZ)] * 2,
            in_specs=vmem(len(parts)),
            out_specs=vmem(2),
            compiler_params=params(8),
            name="pack_rows",
        )(*parts)
        above = lax.ppermute(low, ("xl", "co"), inverse)
        below = lax.ppermute(high, ("xl", "co"), around)
        return below, above

    own = (rhs, inv)
    twin, relay, first, second = [], [], [], []
    for array in range(2):
        twin.append(lax.ppermute(own[array], "xh", [(0, 1), (1, 0)]))
    outer_relay = lax.ppermute(high_half, ("y", "xh"), pairs)
    outer_twin = lax.ppermute(low_half, ("y", "xh"), back)
    first_sums = pl.pallas_call(
        first_kernel,
        out_shape=struct(SK, 8, 128),
        in_specs=vmem(2),
        out_specs=vmem(1)[0],
        compiler_params=params(8),
        cost_estimate=cost(3_000_000),
        name="first_sketch",
    )(right_side, sketch_matrix)
    for array in range(2):
        relay.append(lax.ppermute(twin[array], ("y", "xh"), pairs))
        first.append(pack(FIRST, ("own", "twin"), own[array], twin[array]))
    for array in range(2):
        blocks = (relay[array], outer_relay[array], outer_twin[array])
        second.append(pack(SECOND, ("relay", "outer_relay", "outer_twin"), *blocks))
    parts = (
        *own, *twin, *relay, outer_relay, outer_twin,
        first[0][0], first[1][0], first[0][1], first[1][1],
        second[0][0], second[1][0], second[0][1], second[1][1],
    )
    low, high = pl.pallas_call(
        pack_columns_kernel,
        out_shape=[struct(2, 2, 64, 128)] * 2,
        in_specs=vmem(N_BLOCKS),
        out_specs=vmem(2),
        compiler_params=params(8),
        name="pack_columns",
    )(*parts)
    above = lax.ppermute(low, "z", inverse)
    below = lax.ppermute(high, "z", around)
    main, edge = pl.pallas_call(
        interior_kernel,
        out_shape=[struct(2 * ITERS, BX, BY, BZ), struct(2, 2, MID, ROWS, 128)],
        in_specs=vmem(N_BLOCKS),
        out_specs=vmem(2),
        scratch_shapes=fields(LAYERS),
        compiler_params=params(20),
        cost_estimate=cost(30_000_000),
        name="interior",
    )(*parts)
    vectors, directions, images = pl.pallas_call(
        edge_kernel,
        out_shape=[struct(ITERS, BX, BY, BZ), struct(ITERS, 2, HALF, BY, 128), struct(128, 128)],
        in_specs=[SMEM_SPEC] + vmem(6),
        out_specs=vmem(3),
        scratch_shapes=fields(MID + 1) + [VMEM((ITERS * SK, 8, 128), F32), VMEM((ITERS, BX, BY, BZ), F32)],
        compiler_params=params(16),
        name="edge",
    )(flip, edge, below, above, sketch_matrix, first_sums, main)

    totals = lax.all_to_all(images, ("y", "xh", "xl", "co", "z"), 0, 0, tiled=True)
    return tuple(
        pl.pallas_call(
            final_kernel,
            out_shape=[struct(BX, BY, BZ)] * 2,
            in_specs=[SMEM_SPEC] + vmem(5),
            out_specs=vmem(2),
            scratch_shapes=[VMEM((BX, BY, BZ), F32)],
            compiler_params=params(8),
            name="combine",
        )(flip, totals, right_side, vectors, main, directions)
    )


def solution(mesh):
    finer = Mesh(mesh.devices.reshape(4, 2, 2, 2, 4), ("y", "xh", "xl", "co", "z"))
    spec = (("y", "xh"), ("xl", "co"), "z")

    return jax.shard_map(
        local,
        mesh=finer,
        in_specs=(P(*spec), P(*spec), P(None, *spec)),
        out_specs=(P(*spec), P(*spec)),
        check_vma=False,
    )
```
